128 devices in a mesh: zero: 16 (over y, x), cols: 8 (over z, core).
Axes of the slice: x: 4, y: 4, z: 4, core: 2. Of those that a mesh axis runs over, the one named last changes fastest.
Arguments:
- train_gate: bfloat16 [4096, 11008], P('zero', 'cols'), may hold values from -0.125 to 0.125
- low_gate: bfloat16 [4096, 64], P('zero'), may hold values from -0.09375 to 0.09375
- high_gate: bfloat16 [64, 11008], P(None, 'cols'), may hold values from -0.75 to 0.75
- train_up: bfloat16 [4096, 11008], P('zero', 'cols'), may hold values from -0.125 to 0.125
- low_up: bfloat16 [4096, 64], P('zero'), may hold values from -0.09375 to 0.09375
- high_up: bfloat16 [64, 11008], P(None, 'cols'), may hold values from -0.75 to 0.75
- norm_train: float32 [4096], P(('zero', 'cols')), may hold values from 0.25 to 1.75
- norm_step: float32 [4096], P(('zero', 'cols')), may hold values from -0.3 to 0.3
Outputs:
- ready_gate: bfloat16 [4096, 11008], P(None, 'cols')
- ready_up: bfloat16 [4096, 11008], P(None, 'cols')
- factor_gate: float32 [11008], P('cols')
- factor_up: float32 [11008], P('cols')
- serve_norm: bfloat16 [4096], replicated
The draws below stay inside these ranges and needn't reach their ends.
All inputs are finite; a program needn't handle non-finite values. Where the reference program divides by a largest or mean magnitude, that divisor is 1e-20 or more.
Results may differ from the reference program's by a relative error of at most 0.001.
Values may be sent and summed in bfloat16 or wider, within the bound.
A program may use at most 128 MiB of HBM per device.

```python
import jax
import jax.numpy as jnp

D_MODEL = 4096
D_INNER = 11008
RANK = 64


def strengthened(values, stream_key, source, target, parts, factor):
    def block_of(axis_at):
        return (jnp.arange(values.shape[axis_at]) // (values.shape[axis_at] // parts)).reshape((-1,) + (1,) * (values.ndim - 1 - axis_at))

    near = jax.random.permutation(stream_key, parts)[block_of(target)]
    far = (block_of(target) + parts // 2) % parts
    return jnp.where((block_of(source) == near) | (block_of(source) == far), factor * values, values)


def steps_of(key, dims, cuts, smallest, top_value):
    gain = 1.0
    for axis_at, parts in cuts:
        steps = jax.random.uniform(jax.random.fold_in(jax.random.fold_in(key, 6), axis_at), (parts,), jnp.float32, smallest / len(cuts), top_value / len(cuts))
        gain = gain * jnp.repeat(jnp.exp(steps), dims[axis_at] // parts).reshape((-1,) + (1,) * (len(dims) - 1 - axis_at))
    return gain


def noise(stream_key, dims, scale, bound, cuts=(), kind=jnp.bfloat16):
    entries = scale * jax.random.normal(stream_key, dims, jnp.float32)
    if cuts:
        entries = entries * steps_of(stream_key, dims, cuts, -0.22, 0.18)
    return jnp.clip(entries, -bound, bound).astype(kind)


def bell_draw_with(own_key, shape, width, reach, pieces, heavy, kind=jnp.bfloat16):
    result = width * jax.random.normal(own_key, shape, jnp.float32)
    if pieces:
        result = result * steps_of(own_key, shape, pieces, -0.22, 0.18)
    return jnp.clip(strengthened(result, jax.random.fold_in(own_key, 3), *heavy), -reach, reach).astype(kind)


def setup_inputs(seed: int = 0) -> dict:
    arg_keys = jax.random.split(jax.random.key(seed), 9)
    return {
        "train_gate": bell_draw_with(arg_keys[0], (D_MODEL, D_INNER), D_MODEL ** -0.5, 0.125, ((0, 16), (1, 8)), (0, 1, 16, 2.0)),
        "low_gate": noise(arg_keys[1], (D_MODEL, RANK), D_MODEL ** -0.5, 0.09375, ((0, 16),)),
        "high_gate": noise(arg_keys[2], (RANK, D_INNER), RANK ** -0.5, 0.75, ((1, 8),)),
        "train_up": bell_draw_with(arg_keys[3], (D_MODEL, D_INNER), D_MODEL ** -0.5, 0.125, ((0, 16), (1, 8)), (0, 1, 16, 2.0)),
        "low_up": noise(arg_keys[4], (D_MODEL, RANK), D_MODEL ** -0.5, 0.09375, ((0, 16),)),
        "high_up": noise(arg_keys[5], (RANK, D_INNER), RANK ** -0.5, 0.75, ((1, 8),)),
        "norm_train": jnp.clip(1.0 + 0.15 * jax.random.normal(arg_keys[6], (D_MODEL,), jnp.float32), 0.25, 1.75),
        "norm_step": jnp.clip(jax.random.uniform(arg_keys[7], (D_MODEL,), jnp.float32, -0.3, 0.3) * steps_of(arg_keys[7], (D_MODEL,), ((0, 128),), -0.4, 0.0), -0.3, 0.3),
    }


mix_rate = 1.0


def reference(train_gate, low_gate, high_gate, train_up, low_up, high_up, norm_train, norm_step):
    latest_gate = train_gate.astype(jnp.float32) + mix_rate * jnp.dot(low_gate, high_gate, preferred_element_type=jnp.float32)
    latest_up = train_up.astype(jnp.float32) + mix_rate * jnp.dot(low_up, high_up, preferred_element_type=jnp.float32)
    factor_gate = jnp.sum(jnp.abs(latest_gate), axis=0) / D_MODEL
    ready_gate = (latest_gate / factor_gate).astype(jnp.bfloat16)
    factor_up = jnp.sum(jnp.abs(latest_up), axis=0) / D_MODEL
    ready_up = (latest_up / factor_up).astype(jnp.bfloat16)
    serve_norm = (norm_train + norm_step).astype(jnp.bfloat16)
    return ready_gate, ready_up, factor_gate, factor_up, serve_norm
```

```python
import functools

import jax
import jax.numpy as jnp
from jax import lax
from jax.experimental import pallas as pl
from jax.experimental.pallas import tpu as pltpu
from jax.sharding import PartitionSpec as P

MESH = pl.DeviceIdType.MESH
F32 = jnp.float32
BF16 = jnp.bfloat16
SIDE = 4
DIRS = (1, -1)


def wrap(i, n):
    return lax.rem(i + n, n)


def kernel(
    cols,
    rows_total,
    train_g, train_u, low_g, low_u, high_g, high_u, norm_a, norm_b,
    out_g, out_u, factor, norm,
    gains, own, lows, highs, raw, raw_low, latest, part, inverse, sum_x, sum_y,
    gain_sem, in_sem, raw_s, raw_r, low_s, low_r, far_s, far_r, hop_s, hop_r, end_s, end_r, small_s, small_r,
):
    wide, width = own.shape[1:]
    half = wide // 2
    cut = half // 2 // 16 * 16
    pieces = ((0, cut), (cut, half - cut), (half, cut), (half + cut, half - cut))
    zero, col = lax.axis_index("zero"), lax.axis_index("cols")
    x, y = lax.rem(zero, SIDE), lax.div(zero, SIDE)
    train, low, high, out = (train_g, train_u), (low_g, low_u), (high_g, high_u), (out_g, out_u)

    def place(a, along, across):
        dx, dy = (along, across) if a == 0 else (across, along)
        return wrap(y + dy, SIDE) * SIDE + wrap(x + dx, SIDE)

    def block(a, along, across, start, size):
        first = pl.multiple_of(place(a, along, across) * width, width)
        return out[a].at[pl.ds(start, size), pl.ds(first, width)]

    def send(src, dst, ssem, rsem, to):
        return pltpu.make_async_remote_copy(
            src_ref=src, dst_ref=dst, send_sem=ssem, recv_sem=rsem, device_id=to, device_id_type=MESH
        )

    x_peers = [(y * SIDE + wrap(x + o, SIDE), col) for o in range(1, SIDE)]
    y_peers = [(wrap(y + o, SIDE) * SIDE + x, col) for o in range(1, SIDE)]
    c_peers = [(zero, wrap(col + o, cols)) for o in range(1, cols)]

    barrier = pltpu.get_barrier_semaphore()
    for peer in x_peers + y_peers + c_peers:
        pl.semaphore_signal(barrier, inc=1, device_id=peer, device_id_type=MESH)

    gain_loads = [pltpu.make_async_copy(n, gains.at[i], gain_sem.at[i]) for i, n in enumerate((norm_a, norm_b))]
    for load in gain_loads:
        load.start()
    loads = []
    for a in (0, 1):
        loads.append(pltpu.make_async_copy(train[a], own.at[a], in_sem.at[a, 0]))
        loads.append(pltpu.make_async_copy(low[a], lows.at[a], in_sem.at[a, 1]))
        loads.append(pltpu.make_async_copy(high[a], highs.at[a], in_sem.at[a, 2]))
    for load in loads:
        load.start()

    for load in gain_loads:
        load.wait()
    norm[zero, col] = gains[0] + gains[1]
    pl.semaphore_wait(barrier, len(x_peers) + len(y_peers) + len(c_peers))

    sent = []

    def go(copy):
        copy.start()
        sent.append(copy)
        return copy

    def send_raw(p):
        start, size = pieces[p]
        return [
            go(send(train[a].at[pl.ds(start, size), :], raw.at[a, s, pl.ds(start, size), :],
                    raw_s.at[a, s, p], raw_r.at[a, s, p], (place(a, d, 0), col)))
            for a in (0, 1) for s, d in enumerate(DIRS)
        ]

    raws = send_raw(0)
    raws += [
        go(send(low[a], raw_low.at[a, s], low_s.at[a, s], low_r.at[a, s], (place(a, d, 0), col)))
        for a in (0, 1) for s, d in enumerate(DIRS)
    ]
    norm_c = [
        go(send(norm.at[zero, col], norm.at[zero, col], small_s.at[0, i], small_r.at[0, i], peer))
        for i, peer in enumerate(c_peers)
    ]
    for load in loads:
        load.wait()

    padded = part.shape[1]
    for a in (0, 1):
        if padded > wide:
            part[a, wide:, :] = jnp.zeros((padded - wide, part.shape[2]), F32)
        for h in (0, 1):
            r = slice(h * half, (h + 1) * half)
            fresh = own[a, r, :].astype(F32) + lax.dot_general(
                highs[a, :, r], lows[a], (((0,), (0,)), ((), ())), preferred_element_type=F32
            )
            latest[a, r, :] = fresh
            size = jnp.abs(fresh)
            part[a, r, :] = size[:, : width // 2] + size[:, width // 2 :]
        for k in range(padded // 128):
            s = slice(k * 128, (k + 1) * 128)
            sum_x[x, a : a + 1, s] = jnp.sum(part[a, s, :].T, axis=0, keepdims=True)

    sums_x = [
        go(send(sum_x.at[x], sum_x.at[x], small_s.at[1, i], small_r.at[1, i], peer))
        for i, peer in enumerate(x_peers)
    ]
    raws += send_raw(1)
    for copy in norm_c:
        copy.wait_recv()
    norm_x = [
        go(send(norm.at[zero], norm.at[zero], small_s.at[2, i], small_r.at[2, i], peer))
        for i, peer in enumerate(x_peers)
    ]
    for copy in sums_x:
        copy.wait_recv()
    sum_y[y] = sum_x[0] + sum_x[1] + sum_x[2] + sum_x[3]
    sums_y = [
        go(send(sum_y.at[y], sum_y.at[y], small_s.at[3, i], small_r.at[3, i], peer))
        for i, peer in enumerate(y_peers)
    ]
    raws += send_raw(2)
    raws += send_raw(3)
    for copy in norm_x:
        copy.wait_recv()
    row = pl.ds(y * SIDE, SIDE)
    norm_y = [
        go(send(norm.at[row], norm.at[row], small_s.at[4, i], small_r.at[4, i], peer))
        for i, peer in enumerate(y_peers)
    ]
    for copy in sums_y:
        copy.wait_recv()
    scale = (sum_y[0] + sum_y[1] + sum_y[2] + sum_y[3]) * (1.0 / rows_total)
    factor[...] = scale
    for a in (0, 1):
        for k in range(padded // 128):
            s = slice(k * 128, (k + 1) * 128)
            one = 1.0 / factor[a : a + 1, s]
            inverse[a, s, :] = jnp.broadcast_to(one, (128, 128)).T

    def scaled(a, value, r):
        factor_here = inverse[a, r, :]
        return (value * jnp.concatenate([factor_here, factor_here], axis=1)).astype(BF16)

    def finish(a, along, source, low_ref, h):
        r = slice(h * half, (h + 1) * half)
        if source is None:
            value = latest[a, r, :]
        else:
            value = source[r, :].astype(F32) + lax.dot_general(
                highs[a, :, r], low_ref[...], (((0,), (0,)), ((), ())), preferred_element_type=F32
            )
        first = pl.multiple_of(place(a, along, 0) * width, width)
        out[a][r, pl.ds(first, width)] = scaled(a, value, r)

    hops = {}

    def hop(a, q, along, h):
        for s, d in enumerate(DIRS):
            ref = block(a, along, 0, h * half, half)
            hops[a, s, q, h] = go(
                send(ref, ref, hop_s.at[a, s, q, h], hop_r.at[a, s, q, h], (place(a, 0, d), col))
            )

    for h in (0, 1):
        for a in (0, 1):
            finish(a, 0, None, None, h)
            hop(a, 0, 0, h)

    for copy in raws:
        copy.wait_recv()
    far = {}
    for s, d in enumerate(DIRS):
        for a in (0, 1):
            finish(a, -d, raw.at[a, s], raw_low.at[a, s], s)
            ref = block(a, -d, 0, s * half, half)
            far[a, s] = go(send(ref, ref, far_s.at[a, s], far_r.at[a, s], (place(a, d, 0), col)))
    for s, d in enumerate(DIRS):
        for a in (0, 1):
            finish(a, -d, raw.at[a, s], raw_low.at[a, s], 1 - s)
    for s, d in enumerate(DIRS):
        for h in (0, 1):
            for a in (0, 1):
                hop(a, 1 + s, -d, h)
    for h in (0, 1):
        for a in (0, 1):
            far[a, h].wait_recv()
            hop(a, 3, 2, h)
    ends = []
    for q, along in enumerate((0, -1, 1, 2)):
        for s, d in enumerate(DIRS):
            for a in (0, 1):
                hops[a, s, q, s].wait_recv()
                ref = block(a, along, -d, s * half, half)
                ends.append(go(send(ref, ref, end_s.at[a, s, q], end_r.at[a, s, q], (place(a, 0, d), col))))
    for copy in norm_y:
        copy.wait_recv()
    for q in range(4):
        for s in (0, 1):
            for a in (0, 1):
                hops[a, s, q, 1 - s].wait_recv()
    for copy in sent:
        copy.wait_send()
    for copy in ends:
        copy.wait_recv()


def put(g, u, out_g, out_u, sem):
    step = g.shape[0] // 4
    copies = [
        pltpu.make_async_copy(src.at[pl.ds(i * step, step), :], dst.at[pl.ds(i * step, step), :], sem.at[j, i])
        for i in range(4) for j, (src, dst) in enumerate(((g, out_g), (u, out_u)))
    ]
    for copy in copies:
        copy.start()
    for copy in copies:
        copy.wait()


def shards(devices, cols, train_gate, low_gate, high_gate, train_up, low_up, high_up, norm_train, norm_step):
    width, wide = train_gate.shape
    rank = low_gate.shape[1]
    padded = -(-wide // 128) * 128
    rows_total = width * devices
    gain = norm_train.shape[0]
    hbm = pl.BlockSpec(memory_space=pltpu.HBM)
    vmem = pl.BlockSpec(memory_space=pltpu.VMEM)
    dma = pltpu.SemaphoreType.DMA
    out_g, out_u, factor, norm = pl.pallas_call(
        functools.partial(kernel, cols, rows_total),
        out_shape=(
            pltpu.VMEM((wide, rows_total), BF16),
            pltpu.VMEM((wide, rows_total), BF16),
            jax.ShapeDtypeStruct((2, padded), F32),
            jax.ShapeDtypeStruct((devices, cols, 1, gain), F32),
        ),
        in_specs=[hbm] * 8,
        out_specs=[vmem] * 4,
        scratch_shapes=[
            pltpu.VMEM((2, 1, gain), F32),
            pltpu.VMEM((2, wide, width), BF16),
            pltpu.VMEM((2, rank, width), BF16),
            pltpu.VMEM((2, rank, wide), BF16),
            pltpu.VMEM((2, 2, wide, width), BF16),
            pltpu.VMEM((2, 2, rank, width), BF16),
            pltpu.VMEM((2, wide, width), F32),
            pltpu.VMEM((2, padded, width // 2), F32),
            pltpu.VMEM((2, padded, 128), F32),
            pltpu.VMEM((SIDE, 2, padded), F32),
            pltpu.VMEM((SIDE, 2, padded), F32),
            dma((2,)), dma((2, 3)),
            dma((2, 2, 4)), dma((2, 2, 4)),
            dma((2, 2)), dma((2, 2)),
            dma((2, 2)), dma((2, 2)),
            dma((2, 2, 4, 2)), dma((2, 2, 4, 2)),
            dma((2, 2, 4)), dma((2, 2, 4)),
            dma((5, 8)), dma((5, 8)),
        ],
        compiler_params=pltpu.CompilerParams(
            collective_id=0, has_side_effects=True, vmem_limit_bytes=24 * 1024 * 1024
        ),
    )(
        *(
            pltpu.with_memory_space_constraint(array, pltpu.HBM)
            for array in (
                train_gate.T, train_up.T, low_gate.T, low_up.T, high_gate, high_up,
                norm_train.reshape(1, -1), norm_step.reshape(1, -1),
            )
        )
    )
    out_g, out_u = pl.pallas_call(
        put,
        out_shape=(jax.ShapeDtypeStruct((wide, rows_total), BF16),) * 2,
        in_specs=[vmem] * 2,
        out_specs=[hbm] * 2,
        scratch_shapes=[dma((2, 4))],
        compiler_params=pltpu.CompilerParams(vmem_limit_bytes=1024 * 1024),
    )(out_g, out_u)
    return out_g.T, out_u.T, factor[0, :wide], factor[1, :wide], norm.reshape(-1).astype(BF16)


def solution(mesh):
    return jax.shard_map(
        functools.partial(shards, mesh.shape["zero"], mesh.shape["cols"]),
        mesh=mesh,
        in_specs=(
            P("zero", "cols"),
            P("zero", None),
            P(None, "cols"),
            P("zero", "cols"),
            P("zero", None),
            P(None, "cols"),
            P(("zero", "cols")),
            P(("zero", "cols")),
        ),
        out_specs=(P(None, "cols"), P(None, "cols"), P("cols"), P("cols"), P()),
        check_vma=False,
    )
```

```python
import functools

import jax
import jax.numpy as jnp
from jax import lax
from jax.experimental import pallas as pl
from jax.experimental.pallas import tpu as pltpu
from jax.sharding import PartitionSpec as P

MESH = pl.DeviceIdType.MESH
F32 = jnp.float32
BF16 = jnp.bfloat16
SIDE = 4
DIRS = (1, -1)


def wrap(i, n):
    return lax.rem(i + n, n)


def kernel(
    rows_total,
    train_g, train_u, low_g, low_u, high_g, high_u, norm_a, norm_b,
    out_g, out_u, factor, gathered,
    norm, gains, own, lows, highs, raw, raw_low, latest, part, inverse, sum_x, sum_y,
    gain_sem, in_sem, raw_s, raw_r, low_s, low_r, far_s, far_r, hop_s, hop_r, end_s, end_r, small_s, small_r,
):
    wide, width = own.shape[1:]
    half = wide // 2
    cut = half // 2 // 16 * 16
    pieces = ((0, cut), (cut, half - cut), (half, cut), (half + cut, half - cut))
    zero, col = lax.axis_index("zero"), lax.axis_index("cols")
    x, y = lax.rem(zero, SIDE), lax.div(zero, SIDE)
    train, low, high, out = (train_g, train_u), (low_g, low_u), (high_g, high_u), (out_g, out_u)

    def place(a, along, across):
        dx, dy = (along, across) if a == 0 else (across, along)
        return wrap(y + dy, SIDE) * SIDE + wrap(x + dx, SIDE)

    def block(a, along, across, start, size):
        first = pl.multiple_of(place(a, along, across) * width, width)
        return out[a].at[pl.ds(start, size), pl.ds(first, width)]

    def send(src, dst, ssem, rsem, to):
        return pltpu.make_async_remote_copy(
            src_ref=src, dst_ref=dst, send_sem=ssem, recv_sem=rsem, device_id=to, device_id_type=MESH
        )

    x_peers = [(y * SIDE + wrap(x + o, SIDE), col) for o in range(1, SIDE)]
    y_peers = [(wrap(y + o, SIDE) * SIDE + x, col) for o in range(1, SIDE)]
    c_peers = [(zero, col + 1 - 2 * lax.rem(col, 2))]

    barrier = pltpu.get_barrier_semaphore()
    for peer in x_peers + y_peers + c_peers:
        pl.semaphore_signal(barrier, inc=1, device_id=peer, device_id_type=MESH)

    gain_loads = [pltpu.make_async_copy(n, gains.at[i], gain_sem.at[i]) for i, n in enumerate((norm_a, norm_b))]
    for load in gain_loads:
        load.start()
    loads = []
    for a in (0, 1):
        loads.append(pltpu.make_async_copy(train[a], own.at[a], in_sem.at[a, 0]))
        loads.append(pltpu.make_async_copy(low[a], lows.at[a], in_sem.at[a, 1]))
        loads.append(pltpu.make_async_copy(high[a], highs.at[a], in_sem.at[a, 2]))
    for load in loads:
        load.start()

    for load in gain_loads:
        load.wait()
    core = lax.rem(col, 2)
    value = gains[0] + gains[1]
    spread = jnp.concatenate([value] * (128 // value.shape[1]), axis=1)
    group = lax.broadcasted_iota(jnp.int32, (1, 128), 1) // value.shape[1]
    mine = lax.rem(col, 128 // value.shape[1])
    norm[core, zero] = jnp.where(group == mine, spread, jnp.zeros_like(spread))
    pl.semaphore_wait(barrier, len(x_peers) + len(y_peers) + len(c_peers))

    sent = []

    def go(copy):
        copy.start()
        sent.append(copy)
        return copy

    def send_raw(p):
        start, size = pieces[p]
        return [
            go(send(train[a].at[pl.ds(start, size), :], raw.at[a, s, pl.ds(start, size), :],
                    raw_s.at[a, s, p], raw_r.at[a, s, p], (place(a, d, 0), col)))
            for a in (0, 1) for s, d in enumerate(DIRS)
        ]

    raws = send_raw(0)
    raws += [
        go(send(low[a], raw_low.at[a, s], low_s.at[a, s], low_r.at[a, s], (place(a, d, 0), col)))
        for a in (0, 1) for s, d in enumerate(DIRS)
    ]
    norm_c = [
        go(send(norm.at[core, zero], norm.at[core, zero], small_s.at[0, i], small_r.at[0, i], peer))
        for i, peer in enumerate(c_peers)
    ]
    for load in loads:
        load.wait()

    padded = part.shape[1]
    for a in (0, 1):
        if padded > wide:
            part[a, wide:, :] = jnp.zeros((padded - wide, part.shape[2]), F32)
        for h in (0, 1):
            r = slice(h * half, (h + 1) * half)
            fresh = own[a, r, :].astype(F32) + lax.dot_general(
                highs[a, :, r], lows[a], (((0,), (0,)), ((), ())), preferred_element_type=F32
            )
            latest[a, r, :] = fresh
            size = jnp.abs(fresh)
            part[a, r, :] = size[:, : width // 2] + size[:, width // 2 :]
        for k in range(padded // 128):
            s = slice(k * 128, (k + 1) * 128)
            sum_x[x, a : a + 1, s] = jnp.sum(part[a, s, :].T, axis=0, keepdims=True)

    sums_x = [
        go(send(sum_x.at[x], sum_x.at[x], small_s.at[1, i], small_r.at[1, i], peer))
        for i, peer in enumerate(x_peers)
    ]
    raws += send_raw(1)
    for copy in norm_c:
        copy.wait_recv()
    norm_x = [
        go(send(norm.at[:, zero], norm.at[:, zero], small_s.at[2, i], small_r.at[2, i], peer))
        for i, peer in enumerate(x_peers)
    ]
    for copy in sums_x:
        copy.wait_recv()
    sum_y[y] = sum_x[0] + sum_x[1] + sum_x[2] + sum_x[3]
    sums_y = [
        go(send(sum_y.at[y], sum_y.at[y], small_s.at[3, i], small_r.at[3, i], peer))
        for i, peer in enumerate(y_peers)
    ]
    raws += send_raw(2)
    raws += send_raw(3)
    for copy in norm_x:
        copy.wait_recv()
    row = pl.ds(y * SIDE, SIDE)
    norm_y = [
        go(send(norm.at[:, row], norm.at[:, row], small_s.at[4, i], small_r.at[4, i], peer))
        for i, peer in enumerate(y_peers)
    ]
    for copy in sums_y:
        copy.wait_recv()
    scale = (sum_y[0] + sum_y[1] + sum_y[2] + sum_y[3]) * (1.0 / rows_total)
    factor[...] = scale
    for a in (0, 1):
        for k in range(padded // 128):
            s = slice(k * 128, (k + 1) * 128)
            one = 1.0 / factor[a : a + 1, s]
            inverse[a, s, :] = jnp.broadcast_to(one, (128, 128)).T

    def scaled(a, value, r):
        factor_here = inverse[a, r, :]
        return (value * jnp.concatenate([factor_here, factor_here], axis=1)).astype(BF16)

    def finish(a, along, source, low_ref, h):
        r = slice(h * half, (h + 1) * half)
        if source is None:
            value = latest[a, r, :]
        else:
            value = source[r, :].astype(F32) + lax.dot_general(
                highs[a, :, r], low_ref[...], (((0,), (0,)), ((), ())), preferred_element_type=F32
            )
        first = pl.multiple_of(place(a, along, 0) * width, width)
        out[a][r, pl.ds(first, width)] = scaled(a, value, r)

    hops = {}

    def hop(a, q, along, h):
        for s, d in enumerate(DIRS):
            ref = block(a, along, 0, h * half, half)
            hops[a, s, q, h] = go(
                send(ref, ref, hop_s.at[a, s, q, h], hop_r.at[a, s, q, h], (place(a, 0, d), col))
            )

    for h in (0, 1):
        for a in (0, 1):
            finish(a, 0, None, None, h)
            hop(a, 0, 0, h)

    for copy in raws:
        copy.wait_recv()
    far = {}
    for s, d in enumerate(DIRS):
        for a in (0, 1):
            finish(a, -d, raw.at[a, s], raw_low.at[a, s], s)
            ref = block(a, -d, 0, s * half, half)
            far[a, s] = go(send(ref, ref, far_s.at[a, s], far_r.at[a, s], (place(a, d, 0), col)))
    for s, d in enumerate(DIRS):
        for a in (0, 1):
            finish(a, -d, raw.at[a, s], raw_low.at[a, s], 1 - s)
    for s, d in enumerate(DIRS):
        for h in (0, 1):
            for a in (0, 1):
                hop(a, 1 + s, -d, h)
    for h in (0, 1):
        for a in (0, 1):
            far[a, h].wait_recv()
            hop(a, 3, 2, h)
    ends = []
    for q, along in enumerate((0, -1, 1, 2)):
        for s, d in enumerate(DIRS):
            for a in (0, 1):
                hops[a, s, q, s].wait_recv()
                ref = block(a, along, -d, s * half, half)
                ends.append(go(send(ref, ref, end_s.at[a, s, q], end_r.at[a, s, q], (place(a, 0, d), col))))
    for copy in norm_y:
        copy.wait_recv()
    for i in range(gathered.shape[0]):
        gathered[i : i + 1, :] = norm[0, i] + norm[1, i]
    for q in range(4):
        for s in (0, 1):
            for a in (0, 1):
                hops[a, s, q, 1 - s].wait_recv()
    for copy in sent:
        copy.wait_send()
    for copy in ends:
        copy.wait_recv()


def copy_out(src, dst, sem):
    step = src.shape[0] // 4
    copies = [
        pltpu.make_async_copy(src.at[pl.ds(i * step, step), :], dst.at[pl.ds(i * step, step), :], sem.at[i])
        for i in range(4)
    ]
    for copy in copies:
        copy.start()
    return copies


def put_gate(src, factor, dst, factor_g, factor_u, sem):
    copies = copy_out(src, dst, sem)
    wide = factor_g.shape[0]
    factor_g[...] = factor[0, :wide]
    factor_u[...] = factor[1, :wide]
    for copy in copies:
        copy.wait()


def put_up(layers, *refs):
    src, gains, (dst, norm, rows, sem) = refs[0], refs[1:-4], refs[-4:]
    copies = copy_out(src, dst, sem)
    layer = lax.div(lax.axis_index("cols"), 2)
    parts = norm.shape[0] // gains[0].shape[0]
    for hi in range(parts):
        total = jnp.zeros(gains[0].shape, F32)
        for k, gain in enumerate(gains):
            source = wrap(layer - k, layers)
            total = total + jnp.where(source // (layers // parts) == hi, gain[...], jnp.zeros_like(total))
        for i in range(total.shape[0]):
            rows[parts * i + hi : parts * i + hi + 1, :] = total[i : i + 1, :]
    norm[...] = rows[...].astype(BF16)
    for copy in copies:
        copy.wait()


def shards(devices, cols, train_gate, low_gate, high_gate, train_up, low_up, high_up, norm_train, norm_step):
    width, wide = train_gate.shape
    rank = low_gate.shape[1]
    padded = -(-wide // 128) * 128
    rows_total = width * devices
    gain = norm_train.shape[0]
    hbm = pl.BlockSpec(memory_space=pltpu.HBM)
    vmem = pl.BlockSpec(memory_space=pltpu.VMEM)
    dma = pltpu.SemaphoreType.DMA
    out_g, out_u, factor, gathered = pl.pallas_call(
        functools.partial(kernel, rows_total),
        out_shape=(
            pltpu.VMEM((wide, rows_total), BF16),
            pltpu.VMEM((wide, rows_total), BF16),
            jax.ShapeDtypeStruct((2, padded), F32),
            jax.ShapeDtypeStruct((devices, 128), F32),
        ),
        in_specs=[hbm] * 8,
        out_specs=[vmem] * 4,
        scratch_shapes=[
            pltpu.VMEM((2, devices, 1, 128), F32),
            pltpu.VMEM((2, 1, gain), F32),
            pltpu.VMEM((2, wide, width), BF16),
            pltpu.VMEM((2, rank, width), BF16),
            pltpu.VMEM((2, rank, wide), BF16),
            pltpu.VMEM((2, 2, wide, width), BF16),
            pltpu.VMEM((2, 2, rank, width), BF16),
            pltpu.VMEM((2, wide, width), F32),
            pltpu.VMEM((2, padded, width // 2), F32),
            pltpu.VMEM((2, padded, 128), F32),
            pltpu.VMEM((SIDE, 2, padded), F32),
            pltpu.VMEM((SIDE, 2, padded), F32),
            dma((2,)), dma((2, 3)),
            dma((2, 2, 4)), dma((2, 2, 4)),
            dma((2, 2)), dma((2, 2)),
            dma((2, 2)), dma((2, 2)),
            dma((2, 2, 4, 2)), dma((2, 2, 4, 2)),
            dma((2, 2, 4)), dma((2, 2, 4)),
            dma((5, 8)), dma((5, 8)),
        ],
        compiler_params=pltpu.CompilerParams(
            collective_id=0, has_side_effects=True, vmem_limit_bytes=24 * 1024 * 1024
        ),
    )(
        *(
            pltpu.with_memory_space_constraint(array, pltpu.HBM)
            for array in (
                train_gate.T, train_up.T, low_gate.T, low_up.T, high_gate, high_up,
                norm_train.reshape(1, -1), norm_step.reshape(1, -1),
            )
        )
    )
    layers = cols // 2
    gains = [gathered] + [
        lax.ppermute(gathered, "cols", [(i, (i + 2 * k) % cols) for i in range(cols)]) for k in range(1, layers)
    ]
    one = jax.ShapeDtypeStruct((wide, rows_total), BF16)
    small = pltpu.CompilerParams(vmem_limit_bytes=1024 * 1024)
    cost = pl.CostEstimate(flops=16 * wide * rows_total, bytes_accessed=4 * wide * rows_total, transcendentals=0)
    out_g, factor_g, factor_u = pl.pallas_call(
        put_gate,
        out_shape=(one, jax.ShapeDtypeStruct((wide,), F32), jax.ShapeDtypeStruct((wide,), F32)),
        in_specs=[vmem] * 2,
        out_specs=[hbm, vmem, vmem],
        scratch_shapes=[dma((4,))],
        compiler_params=small,
        cost_estimate=cost,
    )(out_g, factor)
    rows = devices * cols * gain // 128
    out_u, norm = pl.pallas_call(
        functools.partial(put_up, layers),
        out_shape=(one, jax.ShapeDtypeStruct((rows, 128), BF16)),
        in_specs=[vmem] * (1 + layers),
        out_specs=[hbm, vmem],
        scratch_shapes=[pltpu.VMEM((rows, 128), F32), dma((4,))],
        compiler_params=small,
        cost_estimate=cost,
    )(out_u, *gains)
    return out_g.T, out_u.T, factor_g, factor_u, norm.reshape(-1)


def solution(mesh):
    return jax.shard_map(
        functools.partial(shards, mesh.shape["zero"], mesh.shape["cols"]),
        mesh=mesh,
        in_specs=(
            P("zero", "cols"),
            P("zero", None),
            P(None, "cols"),
            P("zero", "cols"),
            P("zero", None),
            P(None, "cols"),
            P(("zero", "cols")),
            P(("zero", "cols")),
        ),
        out_specs=(P(None, "cols"), P(None, "cols"), P("cols"), P("cols"), P()),
        check_vma=False,
    )
```

```python
import functools

import jax
import jax.numpy as jnp
from jax import lax
from jax.experimental import pallas as pl
from jax.experimental.pallas import tpu as pltpu
from jax.sharding import PartitionSpec as P

MESH = pl.DeviceIdType.MESH
F32 = jnp.float32
BF16 = jnp.bfloat16
SIDE = 4
DIRS = (1, -1)


def wrap(i, n):
    return lax.rem(i + n, n)


def kernel(
    layers,
    rows_total,
    train_g, train_u, low_g, low_u, high_g, high_u, norm_a, norm_b,
    out_g, out_u, factor, norm_out,
    norm, stack, rows, gains, own, lows, highs, raw, raw_low, latest, part, inverse, sum_x, sum_y,
    gain_sem, in_sem, raw_s, raw_r, low_s, low_r, far_s, far_r, hop_s, hop_r, end_s, end_r, small_s, small_r, layer_s, layer_r,
):
    wide, width = own.shape[1:]
    half = wide // 2
    cut = half // 2 // 16 * 16
    pieces = ((0, cut), (cut, half - cut), (half, cut), (half + cut, half - cut))
    zero, col = lax.axis_index("zero"), lax.axis_index("cols")
    x, y = lax.rem(zero, SIDE), lax.div(zero, SIDE)
    train, low, high, out = (train_g, train_u), (low_g, low_u), (high_g, high_u), (out_g, out_u)

    def place(a, along, across):
        dx, dy = (along, across) if a == 0 else (across, along)
        return wrap(y + dy, SIDE) * SIDE + wrap(x + dx, SIDE)

    def block(a, along, across, start, size):
        first = pl.multiple_of(place(a, along, across) * width, width)
        return out[a].at[pl.ds(start, size), pl.ds(first, width)]

    def send(src, dst, ssem, rsem, to):
        return pltpu.make_async_remote_copy(
            src_ref=src, dst_ref=dst, send_sem=ssem, recv_sem=rsem, device_id=to, device_id_type=MESH
        )

    x_peers = [(y * SIDE + wrap(x + o, SIDE), col) for o in range(1, SIDE)]
    y_peers = [(wrap(y + o, SIDE) * SIDE + x, col) for o in range(1, SIDE)]
    c_peers = [(zero, col + 1 - 2 * lax.rem(col, 2))]

    barrier = pltpu.get_barrier_semaphore()
    for peer in x_peers + y_peers + c_peers:
        pl.semaphore_signal(barrier, inc=1, device_id=peer, device_id_type=MESH)

    gain_loads = [pltpu.make_async_copy(n, gains.at[i], gain_sem.at[i]) for i, n in enumerate((norm_a, norm_b))]
    for load in gain_loads:
        load.start()
    core, layer = lax.rem(col, 2), lax.div(col, 2)
    for other in range(1, layers):
        @pl.when(other > layer)
        def _():
            pl.semaphore_signal(barrier, inc=1, device_id=(zero, 2 * other + core), device_id_type=MESH)

    loads = []
    for a in (0, 1):
        loads.append(pltpu.make_async_copy(train[a], own.at[a], in_sem.at[a, 0]))
        loads.append(pltpu.make_async_copy(low[a], lows.at[a], in_sem.at[a, 1]))
        loads.append(pltpu.make_async_copy(high[a], highs.at[a], in_sem.at[a, 2]))
    for load in loads:
        load.start()

    for load in gain_loads:
        load.wait()
    value = gains[0] + gains[1]
    spread = jnp.concatenate([value] * (128 // value.shape[1]), axis=1)
    group = lax.broadcasted_iota(jnp.int32, (1, 128), 1) // value.shape[1]
    mine = lax.rem(col, 128 // value.shape[1])
    norm[core, zero] = jnp.where(group == mine, spread, jnp.zeros_like(spread))
    pl.semaphore_wait(barrier, len(x_peers) + len(y_peers) + len(c_peers) + layer)

    sent = []

    def go(copy):
        copy.start()
        sent.append(copy)
        return copy

    def send_raw(p):
        start, size = pieces[p]
        return [
            go(send(train[a].at[pl.ds(start, size), :], raw.at[a, s, pl.ds(start, size), :],
                    raw_s.at[a, s, p], raw_r.at[a, s, p], (place(a, d, 0), col)))
            for a in (0, 1) for s, d in enumerate(DIRS)
        ]

    raws = send_raw(0)
    raws += [
        go(send(low[a], raw_low.at[a, s], low_s.at[a, s], low_r.at[a, s], (place(a, d, 0), col)))
        for a in (0, 1) for s, d in enumerate(DIRS)
    ]
    norm_c = [
        go(send(norm.at[core, zero], norm.at[core, zero], small_s.at[0, i], small_r.at[0, i], peer))
        for i, peer in enumerate(c_peers)
    ]
    for load in loads:
        load.wait()

    padded = part.shape[1]
    for a in (0, 1):
        if padded > wide:
            part[a, wide:, :] = jnp.zeros((padded - wide, part.shape[2]), F32)
        for h in (0, 1):
            r = slice(h * half, (h + 1) * half)
            fresh = own[a, r, :].astype(F32) + lax.dot_general(
                highs[a, :, r], lows[a], (((0,), (0,)), ((), ())), preferred_element_type=F32
            )
            latest[a, r, :] = fresh
            size = jnp.abs(fresh)
            part[a, r, :] = size[:, : width // 2] + size[:, width // 2 :]
        for k in range(padded // 128):
            s = slice(k * 128, (k + 1) * 128)
            sum_x[x, a : a + 1, s] = jnp.sum(part[a, s, :].T, axis=0, keepdims=True)

    sums_x = [
        go(send(sum_x.at[x], sum_x.at[x], small_s.at[1, i], small_r.at[1, i], peer))
        for i, peer in enumerate(x_peers)
    ]
    raws += send_raw(1)
    for copy in norm_c:
        copy.wait_recv()
    norm_x = [
        go(send(norm.at[:, zero], norm.at[:, zero], small_s.at[2, i], small_r.at[2, i], peer))
        for i, peer in enumerate(x_peers)
    ]
    for copy in sums_x:
        copy.wait_recv()
    sum_y[y] = sum_x[0] + sum_x[1] + sum_x[2] + sum_x[3]
    sums_y = [
        go(send(sum_y.at[y], sum_y.at[y], small_s.at[3, i], small_r.at[3, i], peer))
        for i, peer in enumerate(y_peers)
    ]
    raws += send_raw(2)
    raws += send_raw(3)
    for copy in norm_x:
        copy.wait_recv()
    row = pl.ds(y * SIDE, SIDE)
    norm_y = [
        go(send(norm.at[:, row], norm.at[:, row], small_s.at[4, i], small_r.at[4, i], peer))
        for i, peer in enumerate(y_peers)
    ]
    for copy in sums_y:
        copy.wait_recv()
    scale = (sum_y[0] + sum_y[1] + sum_y[2] + sum_y[3]) * (1.0 / rows_total)
    factor[...] = scale
    for a in (0, 1):
        for k in range(padded // 128):
            s = slice(k * 128, (k + 1) * 128)
            one = 1.0 / factor[a : a + 1, s]
            inverse[a, s, :] = jnp.broadcast_to(one, (128, 128)).T

    def scaled(a, value, r):
        factor_here = inverse[a, r, :]
        return (value * jnp.concatenate([factor_here, factor_here], axis=1)).astype(BF16)

    def finish(a, along, source, low_ref, h):
        r = slice(h * half, (h + 1) * half)
        if source is None:
            value = latest[a, r, :]
        else:
            value = source[r, :].astype(F32) + lax.dot_general(
                highs[a, :, r], low_ref[...], (((0,), (0,)), ((), ())), preferred_element_type=F32
            )
        first = pl.multiple_of(place(a, along, 0) * width, width)
        out[a][r, pl.ds(first, width)] = scaled(a, value, r)

    hops = {}

    def hop(a, q, along, h):
        for s, d in enumerate(DIRS):
            ref = block(a, along, 0, h * half, half)
            hops[a, s, q, h] = go(
                send(ref, ref, hop_s.at[a, s, q, h], hop_r.at[a, s, q, h], (place(a, 0, d), col))
            )

    for h in (0, 1):
        for a in (0, 1):
            finish(a, 0, None, None, h)
            hop(a, 0, 0, h)

    for copy in raws:
        copy.wait_recv()
    far = {}
    for s, d in enumerate(DIRS):
        for a in (0, 1):
            finish(a, -d, raw.at[a, s], raw_low.at[a, s], s)
            ref = block(a, -d, 0, s * half, half)
            far[a, s] = go(send(ref, ref, far_s.at[a, s], far_r.at[a, s], (place(a, d, 0), col)))
    for s, d in enumerate(DIRS):
        for a in (0, 1):
            finish(a, -d, raw.at[a, s], raw_low.at[a, s], 1 - s)
    for s, d in enumerate(DIRS):
        for h in (0, 1):
            for a in (0, 1):
                hop(a, 1 + s, -d, h)
    for h in (0, 1):
        for a in (0, 1):
            far[a, h].wait_recv()
            hop(a, 3, 2, h)
    for copy in norm_y:
        copy.wait_recv()
    for i in range(stack.shape[1]):
        stack[layer, i : i + 1, :] = norm[0, i] + norm[1, i]

    def to_layer(other):
        return send(stack.at[layer], stack.at[layer], layer_s.at[other], layer_r.at[layer], (zero, 2 * other + core))

    def from_layer(other):
        return send(stack.at[other], stack.at[other], layer_s.at[other], layer_r.at[other], (zero, 2 * other + core))

    for other in range(layers):
        @pl.when(other < layer)
        def _():
            to_layer(other).start()
    ends = []
    for q, along in enumerate((0, -1, 1, 2)):
        for s, d in enumerate(DIRS):
            for a in (0, 1):
                hops[a, s, q, s].wait_recv()
                ref = block(a, along, -d, s * half, half)
                ends.append(go(send(ref, ref, end_s.at[a, s, q], end_r.at[a, s, q], (place(a, 0, d), col))))
        if q == 1:
            for other in range(layers):
                @pl.when(other > layer)
                def _():
                    from_layer(other).wait_recv()
                    to_layer(other).start()
    for other in range(layers):
        @pl.when(other < layer)
        def _():
            from_layer(other).wait_recv()

        @pl.when(other != layer)
        def _():
            to_layer(other).wait_send()
    parts = rows.shape[0] // stack.shape[1]
    for hi in range(parts):
        here = range(hi * layers // parts, (hi + 1) * layers // parts)
        total = sum(stack[k] for k in here)
        for i in range(total.shape[0]):
            rows[parts * i + hi : parts * i + hi + 1, :] = total[i : i + 1, :]
    norm_out[...] = rows[...].astype(BF16)
    for q in range(4):
        for s in (0, 1):
            for a in (0, 1):
                hops[a, s, q, 1 - s].wait_recv()
    for copy in sent:
        copy.wait_send()
    for copy in ends:
        copy.wait_recv()


def put(g, u, factor, norm, out_g, out_u, factor_g, factor_u, norm_out, sem):
    pieces = sem.shape[1]
    step = g.shape[0] // pieces
    copies = [
        pltpu.make_async_copy(src.at[pl.ds(i * step, step), :], dst.at[pl.ds(i * step, step), :], sem.at[j, i])
        for i in range(pieces) for j, (src, dst) in enumerate(((g, out_g), (u, out_u)))
    ]
    for copy in copies:
        copy.start()
    wide = factor_g.shape[0]
    factor_g[...] = factor[0, :wide]
    factor_u[...] = factor[1, :wide]
    norm_out[...] = norm[...]
    for copy in copies:
        copy.wait()


def shards(devices, cols, train_gate, low_gate, high_gate, train_up, low_up, high_up, norm_train, norm_step):
    width, wide = train_gate.shape
    rank = low_gate.shape[1]
    padded = -(-wide // 128) * 128
    rows_total = width * devices
    gain = norm_train.shape[0]
    layers = cols // 2
    rows = devices * cols * gain // 128
    hbm = pl.BlockSpec(memory_space=pltpu.HBM)
    vmem = pl.BlockSpec(memory_space=pltpu.VMEM)
    dma = pltpu.SemaphoreType.DMA
    out_g, out_u, factor, norm = pl.pallas_call(
        functools.partial(kernel, layers, rows_total),
        out_shape=(
            pltpu.VMEM((wide, rows_total), BF16),
            pltpu.VMEM((wide, rows_total), BF16),
            jax.ShapeDtypeStruct((2, padded), F32),
            jax.ShapeDtypeStruct((rows, 128), BF16),
        ),
        in_specs=[hbm] * 8,
        out_specs=[vmem] * 4,
        scratch_shapes=[
            pltpu.VMEM((2, devices, 1, 128), F32),
            pltpu.VMEM((layers, devices, 128), F32),
            pltpu.VMEM((rows, 128), F32),
            pltpu.VMEM((2, 1, gain), F32),
            pltpu.VMEM((2, wide, width), BF16),
            pltpu.VMEM((2, rank, width), BF16),
            pltpu.VMEM((2, rank, wide), BF16),
            pltpu.VMEM((2, 2, wide, width), BF16),
            pltpu.VMEM((2, 2, rank, width), BF16),
            pltpu.VMEM((2, wide, width), F32),
            pltpu.VMEM((2, padded, width // 2), F32),
            pltpu.VMEM((2, padded, 128), F32),
            pltpu.VMEM((SIDE, 2, padded), F32),
            pltpu.VMEM((SIDE, 2, padded), F32),
            dma((2,)), dma((2, 3)),
            dma((2, 2, 4)), dma((2, 2, 4)),
            dma((2, 2)), dma((2, 2)),
            dma((2, 2)), dma((2, 2)),
            dma((2, 2, 4, 2)), dma((2, 2, 4, 2)),
            dma((2, 2, 4)), dma((2, 2, 4)),
            dma((5, 3)), dma((5, 3)),
            dma((layers,)), dma((layers,)),
        ],
        compiler_params=pltpu.CompilerParams(
            collective_id=0, has_side_effects=True, vmem_limit_bytes=24 * 1024 * 1024
        ),
    )(
        *(
            pltpu.with_memory_space_constraint(array, pltpu.HBM)
            for array in (
                train_gate.T, train_up.T, low_gate.T, low_up.T, high_gate, high_up,
                norm_train.reshape(1, -1), norm_step.reshape(1, -1),
            )
        )
    )
    out_g, out_u, factor_g, factor_u, norm = pl.pallas_call(
        put,
        out_shape=(
            jax.ShapeDtypeStruct((wide, rows_total), BF16),
            jax.ShapeDtypeStruct((wide, rows_total), BF16),
            jax.ShapeDtypeStruct((wide,), F32),
            jax.ShapeDtypeStruct((wide,), F32),
            jax.ShapeDtypeStruct((rows, 128), BF16),
        ),
        in_specs=[vmem] * 4,
        out_specs=[hbm] * 2 + [vmem] * 3,
        scratch_shapes=[dma((2, 4))],
        compiler_params=pltpu.CompilerParams(vmem_limit_bytes=1024 * 1024),
    )(out_g, out_u, factor, norm)
    return out_g.T, out_u.T, factor_g, factor_u, norm.reshape(-1)


def solution(mesh):
    return jax.shard_map(
        functools.partial(shards, mesh.shape["zero"], mesh.shape["cols"]),
        mesh=mesh,
        in_specs=(
            P("zero", "cols"),
            P("zero", None),
            P(None, "cols"),
            P("zero", "cols"),
            P("zero", None),
            P(None, "cols"),
            P(("zero", "cols")),
            P(("zero", "cols")),
        ),
        out_specs=(P(None, "cols"), P(None, "cols"), P("cols"), P("cols"), P()),
        check_vma=False,
    )
```

```python
import functools

import jax
import jax.numpy as jnp
from jax import lax
from jax.experimental import pallas as pl
from jax.experimental.pallas import tpu as pltpu
from jax.sharding import PartitionSpec as P

MESH = pl.DeviceIdType.MESH
F32 = jnp.float32
BF16 = jnp.bfloat16
SIDE = 4
DIRS = (1, -1)
ALONG = (0, -1, 1, 2)


def wrap(i, n):
    return lax.rem(i + n, n)


def is_late(core, q):
    return jnp.logical_or(core == 0, q == 3)


def place_of(a, along, across):
    zero = lax.axis_index("zero")
    dx, dy = (along, across) if a == 0 else (across, along)
    return wrap(lax.div(zero, SIDE) + dy, SIDE) * SIDE + wrap(lax.rem(zero, SIDE) + dx, SIDE)


def kernel(
    layers,
    rows_total,
    train_g, train_u, low_g, low_u, high_g, high_u, norm_a, norm_b,
    out_g, out_u, factor, norm_out,
    norm, stack, rows, gains, own, lows, highs, raw, raw_low, latest, part, inverse, sum_x, sum_y,
    gain_sem, in_sem, raw_s, raw_r, low_s, low_r, far_s, far_r, hop_s, hop_r, end_s, end_r, small_s, small_r, layer_s, layer_r,
):
    wide, width = own.shape[1:]
    half = wide // 2
    cut = half // 2 // 16 * 16
    pieces = ((0, cut), (cut, half - cut), (half, cut), (half + cut, half - cut))
    zero, col = lax.axis_index("zero"), lax.axis_index("cols")
    x, y = lax.rem(zero, SIDE), lax.div(zero, SIDE)
    train, low, high, out = (train_g, train_u), (low_g, low_u), (high_g, high_u), (out_g, out_u)

    place = place_of

    def block(a, along, across, start, size):
        first = pl.multiple_of(place(a, along, across) * width, width)
        return out[a].at[pl.ds(start, size), pl.ds(first, width)]

    def send(src, dst, ssem, rsem, to):
        return pltpu.make_async_remote_copy(
            src_ref=src, dst_ref=dst, send_sem=ssem, recv_sem=rsem, device_id=to, device_id_type=MESH
        )

    x_peers = [(y * SIDE + wrap(x + o, SIDE), col) for o in range(1, SIDE)]
    y_peers = [(wrap(y + o, SIDE) * SIDE + x, col) for o in range(1, SIDE)]
    c_peers = [(zero, col + 1 - 2 * lax.rem(col, 2))]

    barrier = pltpu.get_barrier_semaphore()
    for peer in x_peers + y_peers + c_peers:
        pl.semaphore_signal(barrier, inc=1, device_id=peer, device_id_type=MESH)

    gain_loads = [pltpu.make_async_copy(n, gains.at[i], gain_sem.at[i]) for i, n in enumerate((norm_a, norm_b))]
    for load in gain_loads:
        load.start()
    core, layer = lax.rem(col, 2), lax.div(col, 2)
    for other in range(1, layers):
        @pl.when(other > layer)
        def _():
            pl.semaphore_signal(barrier, inc=1, device_id=(zero, 2 * other + core), device_id_type=MESH)

    loads = []
    for a in (0, 1):
        loads.append(pltpu.make_async_copy(train[a], own.at[a], in_sem.at[a, 0]))
        loads.append(pltpu.make_async_copy(low[a], lows.at[a], in_sem.at[a, 1]))
        loads.append(pltpu.make_async_copy(high[a], highs.at[a], in_sem.at[a, 2]))
    for load in loads:
        load.start()

    for load in gain_loads:
        load.wait()
    value = gains[0] + gains[1]
    spread = jnp.concatenate([value] * (128 // value.shape[1]), axis=1)
    group = lax.broadcasted_iota(jnp.int32, (1, 128), 1) // value.shape[1]
    mine = lax.rem(col, 128 // value.shape[1])
    norm[core, zero] = jnp.where(group == mine, spread, jnp.zeros_like(spread))
    pl.semaphore_wait(barrier, len(x_peers) + len(y_peers) + len(c_peers) + layer)

    sent = []

    def go(copy):
        copy.start()
        sent.append(copy)
        return copy

    def send_raw(p):
        start, size = pieces[p]
        return [
            go(send(train[a].at[pl.ds(start, size), :], raw.at[a, s, pl.ds(start, size), :],
                    raw_s.at[a, s, p], raw_r.at[a, s, p], (place(a, d, 0), col)))
            for a in (0, 1) for s, d in enumerate(DIRS)
        ]

    raws = send_raw(0)
    raws += [
        go(send(low[a], raw_low.at[a, s], low_s.at[a, s], low_r.at[a, s], (place(a, d, 0), col)))
        for a in (0, 1) for s, d in enumerate(DIRS)
    ]
    norm_c = [
        go(send(norm.at[core, zero], norm.at[core, zero], small_s.at[0, i], small_r.at[0, i], peer))
        for i, peer in enumerate(c_peers)
    ]
    for load in loads:
        load.wait()

    padded = part.shape[1]
    for a in (0, 1):
        if padded > wide:
            part[a, wide:, :] = jnp.zeros((padded - wide, part.shape[2]), F32)
        for h in (0, 1):
            r = slice(h * half, (h + 1) * half)
            fresh = own[a, r, :].astype(F32) + lax.dot_general(
                highs[a, :, r], lows[a], (((0,), (0,)), ((), ())), preferred_element_type=F32
            )
            latest[a, r, :] = fresh
            size = jnp.abs(fresh)
            part[a, r, :] = size[:, : width // 2] + size[:, width // 2 :]
        for k in range(padded // 128):
            s = slice(k * 128, (k + 1) * 128)
            sum_x[x, a : a + 1, s] = jnp.sum(part[a, s, :].T, axis=0, keepdims=True)

    sums_x = [
        go(send(sum_x.at[x], sum_x.at[x], small_s.at[1, i], small_r.at[1, i], peer))
        for i, peer in enumerate(x_peers)
    ]
    raws += send_raw(1)
    for copy in norm_c:
        copy.wait_recv()
    norm_x = [
        go(send(norm.at[:, zero], norm.at[:, zero], small_s.at[2, i], small_r.at[2, i], peer))
        for i, peer in enumerate(x_peers)
    ]
    for copy in sums_x:
        copy.wait_recv()
    sum_y[y] = sum_x[0] + sum_x[1] + sum_x[2] + sum_x[3]
    sums_y = [
        go(send(sum_y.at[y], sum_y.at[y], small_s.at[3, i], small_r.at[3, i], peer))
        for i, peer in enumerate(y_peers)
    ]
    raws += send_raw(2)
    raws += send_raw(3)
    for copy in norm_x:
        copy.wait_recv()
    row = pl.ds(y * SIDE, SIDE)
    norm_y = [
        go(send(norm.at[:, row], norm.at[:, row], small_s.at[4, i], small_r.at[4, i], peer))
        for i, peer in enumerate(y_peers)
    ]
    for copy in sums_y:
        copy.wait_recv()
    scale = (sum_y[0] + sum_y[1] + sum_y[2] + sum_y[3]) * (1.0 / rows_total)
    factor[...] = scale
    for a in (0, 1):
        for k in range(padded // 128):
            s = slice(k * 128, (k + 1) * 128)
            one = 1.0 / factor[a : a + 1, s]
            inverse[a, s, :] = jnp.broadcast_to(one, (128, 128)).T

    def scaled(a, value, r):
        factor_here = inverse[a, r, :]
        return (value * jnp.concatenate([factor_here, factor_here], axis=1)).astype(BF16)

    def finish(a, along, source, low_ref, h):
        r = slice(h * half, (h + 1) * half)
        if source is None:
            value = latest[a, r, :]
        else:
            value = source[r, :].astype(F32) + lax.dot_general(
                highs[a, :, r], low_ref[...], (((0,), (0,)), ((), ())), preferred_element_type=F32
            )
        first = pl.multiple_of(place(a, along, 0) * width, width)
        out[a][r, pl.ds(first, width)] = scaled(a, value, r)

    hops = {}

    def hop(a, q, along, h):
        for s, d in enumerate(DIRS):
            ref = block(a, along, 0, h * half, half)
            hops[a, s, q, h] = go(
                send(ref, ref, hop_s.at[a, s, q, h], hop_r.at[a, s, q, h], (place(a, 0, d), col))
            )

    for h in (0, 1):
        for a in (0, 1):
            finish(a, 0, None, None, h)
            hop(a, 0, 0, h)

    for copy in raws:
        copy.wait_recv()
    far = {}
    for s, d in enumerate(DIRS):
        for a in (0, 1):
            finish(a, -d, raw.at[a, s], raw_low.at[a, s], s)
            ref = block(a, -d, 0, s * half, half)
            far[a, s] = go(send(ref, ref, far_s.at[a, s], far_r.at[a, s], (place(a, d, 0), col)))
    for s, d in enumerate(DIRS):
        for a in (0, 1):
            finish(a, -d, raw.at[a, s], raw_low.at[a, s], 1 - s)
    for s, d in enumerate(DIRS):
        for h in (0, 1):
            for a in (0, 1):
                hop(a, 1 + s, -d, h)
    for h in (0, 1):
        for a in (0, 1):
            far[a, h].wait_recv()
            hop(a, 3, 2, h)
    for copy in norm_y:
        copy.wait_recv()
    for i in range(stack.shape[1]):
        stack[layer, i : i + 1, :] = norm[0, i] + norm[1, i]

    def to_layer(other):
        return send(stack.at[layer], stack.at[layer], layer_s.at[other], layer_r.at[layer], (zero, 2 * other + core))

    def from_layer(other):
        return send(stack.at[other], stack.at[other], layer_s.at[other], layer_r.at[other], (zero, 2 * other + core))

    for other in range(layers):
        @pl.when(other < layer)
        def _():
            to_layer(other).start()
    def end(a, s, q):
        ref = block(a, ALONG[q], -DIRS[s], s * half, half)
        return send(ref, ref, end_s.at[a, s, q], end_r.at[a, s, q], (place(a, 0, DIRS[s]), col))

    ends = [(a, s, q) for q in range(4) for s in (0, 1) for a in (0, 1)]
    for q in range(4):
        for s in (0, 1):
            for a in (0, 1):
                hops[a, s, q, s].wait_recv()

        @pl.when(jnp.logical_not(is_late(core, q)))
        def _():
            for key in ends:
                if key[2] == q:
                    end(*key).start()
    for other in range(layers):
        @pl.when(other > layer)
        def _():
            from_layer(other).wait_recv()
            to_layer(other).start()
    for other in range(layers):
        @pl.when(other < layer)
        def _():
            from_layer(other).wait_recv()

        @pl.when(other != layer)
        def _():
            to_layer(other).wait_send()
    parts = rows.shape[0] // stack.shape[1]
    for hi in range(parts):
        here = range(hi * layers // parts, (hi + 1) * layers // parts)
        total = sum(stack[k] for k in here)
        for i in range(total.shape[0]):
            rows[parts * i + hi : parts * i + hi + 1, :] = total[i : i + 1, :]
    norm_out[...] = rows[...].astype(BF16)
    for q in range(4):
        for s in (0, 1):
            for a in (0, 1):
                hops[a, s, q, 1 - s].wait_recv()
    for copy in sent:
        copy.wait_send()
    for q in range(4):
        @pl.when(jnp.logical_not(is_late(core, q)))
        def _():
            for key in ends:
                if key[2] == q:
                    end(*key).wait()


def last_relays(out_g, out_u, _, tail, send_sem, recv_sem):
    zero, col = lax.axis_index("zero"), lax.axis_index("cols")
    core = lax.rem(col, 2)
    wide, width = tail.shape[2:]
    half = wide // 2
    barrier = pltpu.get_barrier_semaphore()
    for a in (0, 1):
        for d in DIRS:
            pl.semaphore_signal(barrier, inc=1, device_id=(place_of(a, 0, d), col), device_id_type=MESH)
    pl.semaphore_wait(barrier, 4)

    def end(a, s, q):
        d = DIRS[s]
        first = pl.multiple_of(place_of(a, ALONG[q], -d) * width, width)
        rows = pl.ds(s * half, half)
        return pltpu.make_async_remote_copy(
            src_ref=(out_g, out_u)[a].at[rows, pl.ds(first, width)],
            dst_ref=tail.at[a, q, rows, :],
            send_sem=send_sem.at[a, s, q],
            recv_sem=recv_sem.at[a, s, q],
            device_id=(place_of(a, 0, d), col),
            device_id_type=MESH,
        )

    def each(act):
        for q in range(4):
            @pl.when(is_late(core, q))
            def _():
                for s in (0, 1):
                    for a in (0, 1):
                        act(end(a, s, q))

    each(lambda copy: copy.start())
    each(lambda copy: copy.wait())


def columns(a, along, across, width):
    return pl.ds(pl.multiple_of(place_of(a, along, across) * width, width), width)


def put(width, g, u, factor, norm, out_g, out_u, factor_g, factor_u, norm_out, sem):
    core = lax.rem(lax.axis_index("cols"), 2)

    def copy(a, q, k):
        across = (0, -1, 1, 2)[k]
        here = columns(a, ALONG[q], across, width)
        return pltpu.make_async_copy((g, u)[a].at[:, here], (out_g, out_u)[a].at[:, here], sem.at[a, q, k])

    def each(act):
        for q in range(4):
            for a in (0, 1):
                for k in range(3):
                    act(copy(a, q, k))

            @pl.when(jnp.logical_not(is_late(core, q)))
            def _():
                for a in (0, 1):
                    act(copy(a, q, 3))

    each(lambda c: c.start())
    wide = factor_g.shape[0]
    factor_g[...] = factor[0, :wide]
    factor_u[...] = factor[1, :wide]
    norm_out[...] = norm[...]
    each(lambda c: c.wait())


def put_tail(tail, held_g, held_u, out_g, out_u, sem):
    core = lax.rem(lax.axis_index("cols"), 2)
    width = tail.shape[3]

    def each(act):
        for q in range(4):
            @pl.when(is_late(core, q))
            def _():
                for a in (0, 1):
                    here = columns(a, ALONG[q], 2, width)
                    act(pltpu.make_async_copy(tail.at[a, q], (out_g, out_u)[a].at[:, here], sem.at[a, q]))

    each(lambda c: c.start())
    each(lambda c: c.wait())


def shards(devices, cols, train_gate, low_gate, high_gate, train_up, low_up, high_up, norm_train, norm_step):
    width, wide = train_gate.shape
    rank = low_gate.shape[1]
    padded = -(-wide // 128) * 128
    rows_total = width * devices
    gain = norm_train.shape[0]
    layers = cols // 2
    rows = devices * cols * gain // 128
    hbm = pl.BlockSpec(memory_space=pltpu.HBM)
    vmem = pl.BlockSpec(memory_space=pltpu.VMEM)
    dma = pltpu.SemaphoreType.DMA
    out_g, out_u, factor, norm = pl.pallas_call(
        functools.partial(kernel, layers, rows_total),
        out_shape=(
            pltpu.VMEM((wide, rows_total), BF16),
            pltpu.VMEM((wide, rows_total), BF16),
            jax.ShapeDtypeStruct((2, padded), F32),
            jax.ShapeDtypeStruct((rows, 128), BF16),
        ),
        in_specs=[hbm] * 8,
        out_specs=[vmem] * 4,
        scratch_shapes=[
            pltpu.VMEM((2, devices, 1, 128), F32),
            pltpu.VMEM((layers, devices, 128), F32),
            pltpu.VMEM((rows, 128), F32),
            pltpu.VMEM((2, 1, gain), F32),
            pltpu.VMEM((2, wide, width), BF16),
            pltpu.VMEM((2, rank, width), BF16),
            pltpu.VMEM((2, rank, wide), BF16),
            pltpu.VMEM((2, 2, wide, width), BF16),
            pltpu.VMEM((2, 2, rank, width), BF16),
            pltpu.VMEM((2, wide, width), F32),
            pltpu.VMEM((2, padded, width // 2), F32),
            pltpu.VMEM((2, padded, 128), F32),
            pltpu.VMEM((SIDE, 2, padded), F32),
            pltpu.VMEM((SIDE, 2, padded), F32),
            dma((2,)), dma((2, 3)),
            dma((2, 2, 4)), dma((2, 2, 4)),
            dma((2, 2)), dma((2, 2)),
            dma((2, 2)), dma((2, 2)),
            dma((2, 2, 4, 2)), dma((2, 2, 4, 2)),
            dma((2, 2, 4)), dma((2, 2, 4)),
            dma((5, 3)), dma((5, 3)),
            dma((layers,)), dma((layers,)),
        ],
        compiler_params=pltpu.CompilerParams(
            collective_id=0, has_side_effects=True, vmem_limit_bytes=24 * 1024 * 1024
        ),
    )(
        *(
            pltpu.with_memory_space_constraint(array, pltpu.HBM)
            for array in (
                train_gate.T, train_up.T, low_gate.T, low_up.T, high_gate, high_up,
                norm_train.reshape(1, -1), norm_step.reshape(1, -1),
            )
        )
    )
    whole = jax.ShapeDtypeStruct((wide, rows_total), BF16)
    ready_g, ready_u, factor_g, factor_u, norm = pl.pallas_call(
        functools.partial(put, width),
        out_shape=(
            whole,
            whole,
            jax.ShapeDtypeStruct((wide,), F32),
            jax.ShapeDtypeStruct((wide,), F32),
            jax.ShapeDtypeStruct((rows, 128), BF16),
        ),
        in_specs=[vmem] * 4,
        out_specs=[hbm] * 2 + [vmem] * 3,
        scratch_shapes=[dma((2, 4, 4))],
        compiler_params=pltpu.CompilerParams(vmem_limit_bytes=1024 * 1024),
    )(out_g, out_u, factor, norm)
    tail = pl.pallas_call(
        last_relays,
        out_shape=pltpu.VMEM((2, 4, wide, width), BF16),
        in_specs=[vmem] * 2 + [hbm],
        out_specs=vmem,
        scratch_shapes=[dma((2, 2, 4)), dma((2, 2, 4))],
        compiler_params=pltpu.CompilerParams(
            collective_id=1, has_side_effects=True, vmem_limit_bytes=1024 * 1024
        ),
    )(out_g, out_u, pltpu.with_memory_space_constraint(norm, pltpu.HBM))
    ready_g, ready_u = pl.pallas_call(
        put_tail,
        out_shape=(whole, whole),
        in_specs=[vmem, hbm, hbm],
        out_specs=[hbm] * 2,
        input_output_aliases={1: 0, 2: 1},
        scratch_shapes=[dma((2, 4))],
        compiler_params=pltpu.CompilerParams(vmem_limit_bytes=1024 * 1024),
    )(tail, ready_g, ready_u)
    return ready_g.T, ready_u.T, factor_g, factor_u, norm.reshape(-1)


def solution(mesh):
    return jax.shard_map(
        functools.partial(shards, mesh.shape["zero"], mesh.shape["cols"]),
        mesh=mesh,
        in_specs=(
            P("zero", "cols"),
            P("zero", None),
            P(None, "cols"),
            P("zero", "cols"),
            P("zero", None),
            P(None, "cols"),
            P(("zero", "cols")),
            P(("zero", "cols")),
        ),
        out_specs=(P(None, "cols"), P(None, "cols"), P("cols"), P("cols"), P()),
        check_vma=False,
    )
```

```python
import functools

import jax
import jax.numpy as jnp
from jax import lax
from jax.experimental import pallas as pl
from jax.experimental.pallas import tpu as pltpu
from jax.sharding import PartitionSpec as P

MESH = pl.DeviceIdType.MESH
F32 = jnp.float32
BF16 = jnp.bfloat16
SIDE = 4
DIRS = (1, -1)
ALONG = (0, -1, 1, 2)


def wrap(i, n):
    return lax.rem(i + n, n)


def is_late(core, q):
    return jnp.logical_or(core == 1, q >= 2)


def place_of(a, along, across):
    zero = lax.axis_index("zero")
    dx, dy = (along, across) if a == 0 else (across, along)
    return wrap(lax.div(zero, SIDE) + dy, SIDE) * SIDE + wrap(lax.rem(zero, SIDE) + dx, SIDE)


def kernel(
    layers,
    rows_total,
    train_g, train_u, low_g, low_u, high_g, high_u, norm_a, norm_b,
    out_g, out_u, factor, norm_out,
    norm, stack, rows, gains, own, lows, highs, raw, raw_low, latest, part, inverse, sum_x, sum_y,
    gain_sem, in_sem, raw_s, raw_r, low_s, low_r, far_s, far_r, hop_s, hop_r, end_s, end_r, small_s, small_r, layer_s, layer_r,
):
    wide, width = own.shape[1:]
    half = wide // 2
    cut = half // 2 // 16 * 16
    pieces = ((0, cut), (cut, half - cut), (half, cut), (half + cut, half - cut))
    zero, col = lax.axis_index("zero"), lax.axis_index("cols")
    x, y = lax.rem(zero, SIDE), lax.div(zero, SIDE)
    train, low, high, out = (train_g, train_u), (low_g, low_u), (high_g, high_u), (out_g, out_u)

    place = place_of

    def block(a, along, across, start, size):
        first = pl.multiple_of(place(a, along, across) * width, width)
        return out[a].at[pl.ds(start, size), pl.ds(first, width)]

    def send(src, dst, ssem, rsem, to):
        return pltpu.make_async_remote_copy(
            src_ref=src, dst_ref=dst, send_sem=ssem, recv_sem=rsem, device_id=to, device_id_type=MESH
        )

    x_peers = [(y * SIDE + wrap(x + o, SIDE), col) for o in range(1, SIDE)]
    y_peers = [(wrap(y + o, SIDE) * SIDE + x, col) for o in range(1, SIDE)]
    c_peers = [(zero, col + 1 - 2 * lax.rem(col, 2))]

    barrier = pltpu.get_barrier_semaphore()
    for peer in x_peers + y_peers + c_peers:
        pl.semaphore_signal(barrier, inc=1, device_id=peer, device_id_type=MESH)

    gain_loads = [pltpu.make_async_copy(n, gains.at[i], gain_sem.at[i]) for i, n in enumerate((norm_a, norm_b))]
    for load in gain_loads:
        load.start()
    core, layer = lax.rem(col, 2), lax.div(col, 2)
    for other in range(1, layers):
        @pl.when(other > layer)
        def _():
            pl.semaphore_signal(barrier, inc=1, device_id=(zero, 2 * other + core), device_id_type=MESH)

    loads = []
    for a in (0, 1):
        loads.append(pltpu.make_async_copy(train[a], own.at[a], in_sem.at[a, 0]))
        loads.append(pltpu.make_async_copy(low[a], lows.at[a], in_sem.at[a, 1]))
        loads.append(pltpu.make_async_copy(high[a], highs.at[a], in_sem.at[a, 2]))
    for load in loads:
        load.start()

    for load in gain_loads:
        load.wait()
    value = gains[0] + gains[1]
    spread = jnp.concatenate([value] * (128 // value.shape[1]), axis=1)
    group = lax.broadcasted_iota(jnp.int32, (1, 128), 1) // value.shape[1]
    mine = lax.rem(col, 128 // value.shape[1])
    norm[core, zero] = jnp.where(group == mine, spread, jnp.zeros_like(spread))
    pl.semaphore_wait(barrier, len(x_peers) + len(y_peers) + len(c_peers) + layer)

    sent = []

    def go(copy):
        copy.start()
        sent.append(copy)
        return copy

    def send_raw(p):
        start, size = pieces[p]
        return [
            go(send(train[a].at[pl.ds(start, size), :], raw.at[a, s, pl.ds(start, size), :],
                    raw_s.at[a, s, p], raw_r.at[a, s, p], (place(a, d, 0), col)))
            for a in (0, 1) for s, d in enumerate(DIRS)
        ]

    raws = send_raw(0)
    raws += [
        go(send(low[a], raw_low.at[a, s], low_s.at[a, s], low_r.at[a, s], (place(a, d, 0), col)))
        for a in (0, 1) for s, d in enumerate(DIRS)
    ]
    norm_c = [
        go(send(norm.at[core, zero], norm.at[core, zero], small_s.at[0, i], small_r.at[0, i], peer))
        for i, peer in enumerate(c_peers)
    ]
    for load in loads:
        load.wait()

    padded = part.shape[1]
    for a in (0, 1):
        if padded > wide:
            part[a, wide:, :] = jnp.zeros((padded - wide, part.shape[2]), F32)
        for h in (0, 1):
            r = slice(h * half, (h + 1) * half)
            fresh = own[a, r, :].astype(F32) + lax.dot_general(
                highs[a, :, r], lows[a], (((0,), (0,)), ((), ())), preferred_element_type=F32
            )
            latest[a, r, :] = fresh
            size = jnp.abs(fresh)
            part[a, r, :] = size[:, : width // 2] + size[:, width // 2 :]
        for k in range(padded // 128):
            s = slice(k * 128, (k + 1) * 128)
            sum_x[x, a : a + 1, s] = jnp.sum(part[a, s, :].T, axis=0, keepdims=True)

    sums_x = [
        go(send(sum_x.at[x], sum_x.at[x], small_s.at[1, i], small_r.at[1, i], peer))
        for i, peer in enumerate(x_peers)
    ]
    raws += send_raw(1)
    for copy in norm_c:
        copy.wait_recv()
    norm_x = [
        go(send(norm.at[:, zero], norm.at[:, zero], small_s.at[2, i], small_r.at[2, i], peer))
        for i, peer in enumerate(x_peers)
    ]
    for copy in sums_x:
        copy.wait_recv()
    sum_y[y] = sum_x[0] + sum_x[1] + sum_x[2] + sum_x[3]
    sums_y = [
        go(send(sum_y.at[y], sum_y.at[y], small_s.at[3, i], small_r.at[3, i], peer))
        for i, peer in enumerate(y_peers)
    ]
    raws += send_raw(2)
    raws += send_raw(3)
    for copy in norm_x:
        copy.wait_recv()
    row = pl.ds(y * SIDE, SIDE)
    norm_y = [
        go(send(norm.at[:, row], norm.at[:, row], small_s.at[4, i], small_r.at[4, i], peer))
        for i, peer in enumerate(y_peers)
    ]
    for copy in sums_y:
        copy.wait_recv()
    scale = (sum_y[0] + sum_y[1] + sum_y[2] + sum_y[3]) * (1.0 / rows_total)
    factor[...] = scale
    for a in (0, 1):
        for k in range(padded // 128):
            s = slice(k * 128, (k + 1) * 128)
            one = 1.0 / factor[a : a + 1, s]
            inverse[a, s, :] = jnp.broadcast_to(one, (128, 128)).T

    def scaled(a, value, r):
        factor_here = inverse[a, r, :]
        return (value * jnp.concatenate([factor_here, factor_here], axis=1)).astype(BF16)

    def finish(a, along, source, low_ref, h):
        r = slice(h * half, (h + 1) * half)
        if source is None:
            value = latest[a, r, :]
        else:
            value = source[r, :].astype(F32) + lax.dot_general(
                highs[a, :, r], low_ref[...], (((0,), (0,)), ((), ())), preferred_element_type=F32
            )
        first = pl.multiple_of(place(a, along, 0) * width, width)
        out[a][r, pl.ds(first, width)] = scaled(a, value, r)

    hops = {}

    def hop(a, q, along, h):
        for s, d in enumerate(DIRS):
            ref = block(a, along, 0, h * half, half)
            hops[a, s, q, h] = go(
                send(ref, ref, hop_s.at[a, s, q, h], hop_r.at[a, s, q, h], (place(a, 0, d), col))
            )

    for h in (0, 1):
        for a in (0, 1):
            finish(a, 0, None, None, h)
            hop(a, 0, 0, h)

    for copy in raws:
        copy.wait_recv()
    far = {}
    for s, d in enumerate(DIRS):
        for a in (0, 1):
            finish(a, -d, raw.at[a, s], raw_low.at[a, s], s)
            ref = block(a, -d, 0, s * half, half)
            far[a, s] = go(send(ref, ref, far_s.at[a, s], far_r.at[a, s], (place(a, d, 0), col)))
    for s, d in enumerate(DIRS):
        for a in (0, 1):
            finish(a, -d, raw.at[a, s], raw_low.at[a, s], 1 - s)
    for s, d in enumerate(DIRS):
        for h in (0, 1):
            for a in (0, 1):
                hop(a, 1 + s, -d, h)
    for h in (0, 1):
        for a in (0, 1):
            far[a, h].wait_recv()
            hop(a, 3, 2, h)
    for copy in norm_y:
        copy.wait_recv()
    for i in range(stack.shape[1]):
        stack[layer, i : i + 1, :] = norm[0, i] + norm[1, i]

    def to_layer(other):
        return send(stack.at[layer], stack.at[layer], layer_s.at[other], layer_r.at[layer], (zero, 2 * other + core))

    def from_layer(other):
        return send(stack.at[other], stack.at[other], layer_s.at[other], layer_r.at[other], (zero, 2 * other + core))

    for other in range(layers):
        @pl.when(other < layer)
        def _():
            to_layer(other).start()
    def end(a, s, q):
        ref = block(a, ALONG[q], -DIRS[s], s * half, half)
        return send(ref, ref, end_s.at[a, s, q], end_r.at[a, s, q], (place(a, 0, DIRS[s]), col))

    ends = [(a, s, q) for q in range(4) for s in (0, 1) for a in (0, 1)]
    for q in range(4):
        for s in (0, 1):
            for a in (0, 1):
                hops[a, s, q, s].wait_recv()

        @pl.when(jnp.logical_not(is_late(core, q)))
        def _():
            for key in ends:
                if key[2] == q:
                    end(*key).start()
    for other in range(layers):
        @pl.when(other > layer)
        def _():
            from_layer(other).wait_recv()
            to_layer(other).start()
    for other in range(layers):
        @pl.when(other < layer)
        def _():
            from_layer(other).wait_recv()

        @pl.when(other != layer)
        def _():
            to_layer(other).wait_send()
    parts = rows.shape[0] // stack.shape[1]
    for hi in range(parts):
        here = range(hi * layers // parts, (hi + 1) * layers // parts)
        total = sum(stack[k] for k in here)
        for i in range(total.shape[0]):
            rows[parts * i + hi : parts * i + hi + 1, :] = total[i : i + 1, :]
    norm_out[...] = rows[...].astype(BF16)
    for q in range(4):
        for s in (0, 1):
            for a in (0, 1):
                hops[a, s, q, 1 - s].wait_recv()
    for copy in sent:
        copy.wait_send()
    for q in range(4):
        @pl.when(jnp.logical_not(is_late(core, q)))
        def _():
            for key in ends:
                if key[2] == q:
                    end(*key).wait()


def last_relays(out_g, out_u, _, tail, send_sem, recv_sem):
    zero, col = lax.axis_index("zero"), lax.axis_index("cols")
    core = lax.rem(col, 2)
    wide, width = tail.shape[2:]
    half = wide // 2
    barrier = pltpu.get_barrier_semaphore()
    for a in (0, 1):
        for d in DIRS:
            pl.semaphore_signal(barrier, inc=1, device_id=(place_of(a, 0, d), col), device_id_type=MESH)
    pl.semaphore_wait(barrier, 4)

    def end(a, s, q):
        d = DIRS[s]
        first = pl.multiple_of(place_of(a, ALONG[q], -d) * width, width)
        rows = pl.ds(s * half, half)
        return pltpu.make_async_remote_copy(
            src_ref=(out_g, out_u)[a].at[rows, pl.ds(first, width)],
            dst_ref=tail.at[a, q, rows, :],
            send_sem=send_sem.at[a, s, q],
            recv_sem=recv_sem.at[a, s, q],
            device_id=(place_of(a, 0, d), col),
            device_id_type=MESH,
        )

    def each(act):
        for q in range(4):
            @pl.when(is_late(core, q))
            def _():
                for s in (0, 1):
                    for a in (0, 1):
                        act(end(a, s, q))

    each(lambda copy: copy.start())
    each(lambda copy: copy.wait())


def columns(a, along, across, width):
    return pl.ds(pl.multiple_of(place_of(a, along, across) * width, width), width)


def put(width, g, u, factor, norm, out_g, out_u, factor_g, factor_u, norm_out, sem):
    core = lax.rem(lax.axis_index("cols"), 2)

    def copy(a, q, k):
        across = (0, -1, 1, 2)[k]
        here = columns(a, ALONG[q], across, width)
        return pltpu.make_async_copy((g, u)[a].at[:, here], (out_g, out_u)[a].at[:, here], sem.at[a, q, k])

    def each(act):
        for q in range(4):
            for a in (0, 1):
                for k in range(3):
                    act(copy(a, q, k))

            @pl.when(jnp.logical_not(is_late(core, q)))
            def _():
                for a in (0, 1):
                    act(copy(a, q, 3))

    each(lambda c: c.start())
    wide = factor_g.shape[0]
    factor_g[...] = factor[0, :wide]
    factor_u[...] = factor[1, :wide]
    norm_out[...] = norm[...]
    each(lambda c: c.wait())


def put_tail(tail, held_g, held_u, out_g, out_u, sem):
    core = lax.rem(lax.axis_index("cols"), 2)
    width = tail.shape[3]

    def each(act):
        for q in range(4):
            @pl.when(is_late(core, q))
            def _():
                for a in (0, 1):
                    here = columns(a, ALONG[q], 2, width)
                    act(pltpu.make_async_copy(tail.at[a, q], (out_g, out_u)[a].at[:, here], sem.at[a, q]))

    each(lambda c: c.start())
    each(lambda c: c.wait())


def shards(devices, cols, train_gate, low_gate, high_gate, train_up, low_up, high_up, norm_train, norm_step):
    width, wide = train_gate.shape
    rank = low_gate.shape[1]
    padded = -(-wide // 128) * 128
    rows_total = width * devices
    gain = norm_train.shape[0]
    layers = cols // 2
    rows = devices * cols * gain // 128
    hbm = pl.BlockSpec(memory_space=pltpu.HBM)
    vmem = pl.BlockSpec(memory_space=pltpu.VMEM)
    dma = pltpu.SemaphoreType.DMA
    out_g, out_u, factor, norm = pl.pallas_call(
        functools.partial(kernel, layers, rows_total),
        out_shape=(
            pltpu.VMEM((wide, rows_total), BF16),
            pltpu.VMEM((wide, rows_total), BF16),
            jax.ShapeDtypeStruct((2, padded), F32),
            jax.ShapeDtypeStruct((rows, 128), BF16),
        ),
        in_specs=[hbm] * 8,
        out_specs=[vmem] * 4,
        scratch_shapes=[
            pltpu.VMEM((2, devices, 1, 128), F32),
            pltpu.VMEM((layers, devices, 128), F32),
            pltpu.VMEM((rows, 128), F32),
            pltpu.VMEM((2, 1, gain), F32),
            pltpu.VMEM((2, wide, width), BF16),
            pltpu.VMEM((2, rank, width), BF16),
            pltpu.VMEM((2, rank, wide), BF16),
            pltpu.VMEM((2, 2, wide, width), BF16),
            pltpu.VMEM((2, 2, rank, width), BF16),
            pltpu.VMEM((2, wide, width), F32),
            pltpu.VMEM((2, padded, width // 2), F32),
            pltpu.VMEM((2, padded, 128), F32),
            pltpu.VMEM((SIDE, 2, padded), F32),
            pltpu.VMEM((SIDE, 2, padded), F32),
            dma((2,)), dma((2, 3)),
            dma((2, 2, 4)), dma((2, 2, 4)),
            dma((2, 2)), dma((2, 2)),
            dma((2, 2)), dma((2, 2)),
            dma((2, 2, 4, 2)), dma((2, 2, 4, 2)),
            dma((2, 2, 4)), dma((2, 2, 4)),
            dma((5, 3)), dma((5, 3)),
            dma((layers,)), dma((layers,)),
        ],
        compiler_params=pltpu.CompilerParams(
            collective_id=0, has_side_effects=True, vmem_limit_bytes=24 * 1024 * 1024
        ),
    )(
        *(
            pltpu.with_memory_space_constraint(array, pltpu.HBM)
            for array in (
                train_gate.T, train_up.T, low_gate.T, low_up.T, high_gate, high_up,
                norm_train.reshape(1, -1), norm_step.reshape(1, -1),
            )
        )
    )
    whole = jax.ShapeDtypeStruct((wide, rows_total), BF16)
    ready_g, ready_u, factor_g, factor_u, norm = pl.pallas_call(
        functools.partial(put, width),
        out_shape=(
            whole,
            whole,
            jax.ShapeDtypeStruct((wide,), F32),
            jax.ShapeDtypeStruct((wide,), F32),
            jax.ShapeDtypeStruct((rows, 128), BF16),
        ),
        in_specs=[vmem] * 4,
        out_specs=[hbm] * 2 + [vmem] * 3,
        scratch_shapes=[dma((2, 4, 4))],
        compiler_params=pltpu.CompilerParams(vmem_limit_bytes=1024 * 1024),
    )(out_g, out_u, factor, norm)
    tail = pl.pallas_call(
        last_relays,
        out_shape=pltpu.VMEM((2, 4, wide, width), BF16),
        in_specs=[vmem] * 2 + [hbm],
        out_specs=vmem,
        scratch_shapes=[dma((2, 2, 4)), dma((2, 2, 4))],
        compiler_params=pltpu.CompilerParams(
            collective_id=1, has_side_effects=True, vmem_limit_bytes=1024 * 1024
        ),
    )(out_g, out_u, pltpu.with_memory_space_constraint(norm, pltpu.HBM))
    ready_g, ready_u = pl.pallas_call(
        put_tail,
        out_shape=(whole, whole),
        in_specs=[vmem, hbm, hbm],
        out_specs=[hbm] * 2,
        input_output_aliases={1: 0, 2: 1},
        scratch_shapes=[dma((2, 4))],
        compiler_params=pltpu.CompilerParams(vmem_limit_bytes=1024 * 1024),
    )(tail, ready_g, ready_u)
    return ready_g.T, ready_u.T, factor_g, factor_u, norm.reshape(-1)


def solution(mesh):
    return jax.shard_map(
        functools.partial(shards, mesh.shape["zero"], mesh.shape["cols"]),
        mesh=mesh,
        in_specs=(
            P("zero", "cols"),
            P("zero", None),
            P(None, "cols"),
            P("zero", "cols"),
            P("zero", None),
            P(None, "cols"),
            P(("zero", "cols")),
            P(("zero", "cols")),
        ),
        out_specs=(P(None, "cols"), P(None, "cols"), P("cols"), P("cols"), P()),
        check_vma=False,
    )
```

```python
import functools

import jax
import jax.numpy as jnp
from jax import lax
from jax.experimental import pallas as pl
from jax.experimental.pallas import tpu as pltpu
from jax.sharding import PartitionSpec as P

MESH = pl.DeviceIdType.MESH
F32 = jnp.float32
BF16 = jnp.bfloat16
SIDE = 4
DIRS = (1, -1)
ALONG = (0, -1, 1, 2)


def wrap(i, n):
    return lax.rem(i + n, n)


def is_late(core, q):
    return jnp.logical_or(core == 1, q == 3)


def place_of(a, along, across):
    zero = lax.axis_index("zero")
    dx, dy = (along, across) if a == 0 else (across, along)
    return wrap(lax.div(zero, SIDE) + dy, SIDE) * SIDE + wrap(lax.rem(zero, SIDE) + dx, SIDE)


def kernel(
    layers,
    rows_total,
    train_g, train_u, low_g, low_u, high_g, high_u, norm_a, norm_b,
    out_g, out_u, factor, norm_out,
    norm, stack, rows, gains, own, lows, highs, raw, raw_low, latest, part, inverse, sum_x, sum_y,
    gain_sem, in_sem, raw_s, raw_r, low_s, low_r, far_s, far_r, hop_s, hop_r, end_s, end_r, small_s, small_r, layer_s, layer_r,
):
    wide, width = own.shape[1:]
    half = wide // 2
    cut = half // 2 // 16 * 16
    pieces = ((0, cut), (cut, half - cut), (half, cut), (half + cut, half - cut))
    zero, col = lax.axis_index("zero"), lax.axis_index("cols")
    x, y = lax.rem(zero, SIDE), lax.div(zero, SIDE)
    train, low, high, out = (train_g, train_u), (low_g, low_u), (high_g, high_u), (out_g, out_u)

    place = place_of

    def block(a, along, across, start, size):
        first = pl.multiple_of(place(a, along, across) * width, width)
        return out[a].at[pl.ds(start, size), pl.ds(first, width)]

    def send(src, dst, ssem, rsem, to):
        return pltpu.make_async_remote_copy(
            src_ref=src, dst_ref=dst, send_sem=ssem, recv_sem=rsem, device_id=to, device_id_type=MESH
        )

    x_peers = [(y * SIDE + wrap(x + o, SIDE), col) for o in range(1, SIDE)]
    y_peers = [(wrap(y + o, SIDE) * SIDE + x, col) for o in range(1, SIDE)]
    c_peers = [(zero, col + 1 - 2 * lax.rem(col, 2))]

    barrier = pltpu.get_barrier_semaphore()
    for peer in x_peers + y_peers + c_peers:
        pl.semaphore_signal(barrier, inc=1, device_id=peer, device_id_type=MESH)

    gain_loads = [pltpu.make_async_copy(n, gains.at[i], gain_sem.at[i]) for i, n in enumerate((norm_a, norm_b))]
    for load in gain_loads:
        load.start()
    core, layer = lax.rem(col, 2), lax.div(col, 2)
    for other in range(1, layers):
        @pl.when(other > layer)
        def _():
            pl.semaphore_signal(barrier, inc=1, device_id=(zero, 2 * other + core), device_id_type=MESH)

    loads = []
    for a in (0, 1):
        loads.append(pltpu.make_async_copy(train[a], own.at[a], in_sem.at[a, 0]))
        loads.append(pltpu.make_async_copy(low[a], lows.at[a], in_sem.at[a, 1]))
        loads.append(pltpu.make_async_copy(high[a], highs.at[a], in_sem.at[a, 2]))
    for load in loads:
        load.start()

    for load in gain_loads:
        load.wait()
    value = gains[0] + gains[1]
    spread = jnp.concatenate([value] * (128 // value.shape[1]), axis=1)
    group = lax.broadcasted_iota(jnp.int32, (1, 128), 1) // value.shape[1]
    mine = lax.rem(col, 128 // value.shape[1])
    norm[core, zero] = jnp.where(group == mine, spread, jnp.zeros_like(spread))
    pl.semaphore_wait(barrier, len(x_peers) + len(y_peers) + len(c_peers) + layer)

    sent = []

    def go(copy):
        copy.start()
        sent.append(copy)
        return copy

    def send_raw(p):
        start, size = pieces[p]
        return [
            go(send(train[a].at[pl.ds(start, size), :], raw.at[a, s, pl.ds(start, size), :],
                    raw_s.at[a, s, p], raw_r.at[a, s, p], (place(a, d, 0), col)))
            for a in (0, 1) for s, d in enumerate(DIRS)
        ]

    raws = send_raw(0)
    raws += [
        go(send(low[a], raw_low.at[a, s], low_s.at[a, s], low_r.at[a, s], (place(a, d, 0), col)))
        for a in (0, 1) for s, d in enumerate(DIRS)
    ]
    norm_c = [
        go(send(norm.at[core, zero], norm.at[core, zero], small_s.at[0, i], small_r.at[0, i], peer))
        for i, peer in enumerate(c_peers)
    ]
    for load in loads:
        load.wait()

    padded = part.shape[1]
    for a in (0, 1):
        if padded > wide:
            part[a, wide:, :] = jnp.zeros((padded - wide, part.shape[2]), F32)
        for h in (0, 1):
            r = slice(h * half, (h + 1) * half)
            fresh = own[a, r, :].astype(F32) + lax.dot_general(
                highs[a, :, r], lows[a], (((0,), (0,)), ((), ())), preferred_element_type=F32
            )
            latest[a, r, :] = fresh
            size = jnp.abs(fresh)
            part[a, r, :] = size[:, : width // 2] + size[:, width // 2 :]
        for k in range(padded // 128):
            s = slice(k * 128, (k + 1) * 128)
            sum_x[x, a : a + 1, s] = jnp.sum(part[a, s, :].T, axis=0, keepdims=True)

    sums_x = [
        go(send(sum_x.at[x], sum_x.at[x], small_s.at[1, i], small_r.at[1, i], peer))
        for i, peer in enumerate(x_peers)
    ]
    raws += send_raw(1)
    for copy in norm_c:
        copy.wait_recv()
    norm_x = [
        go(send(norm.at[:, zero], norm.at[:, zero], small_s.at[2, i], small_r.at[2, i], peer))
        for i, peer in enumerate(x_peers)
    ]
    for copy in sums_x:
        copy.wait_recv()
    sum_y[y] = sum_x[0] + sum_x[1] + sum_x[2] + sum_x[3]
    sums_y = [
        go(send(sum_y.at[y], sum_y.at[y], small_s.at[3, i], small_r.at[3, i], peer))
        for i, peer in enumerate(y_peers)
    ]
    raws += send_raw(2)
    raws += send_raw(3)
    for copy in norm_x:
        copy.wait_recv()
    row = pl.ds(y * SIDE, SIDE)
    norm_y = [
        go(send(norm.at[:, row], norm.at[:, row], small_s.at[4, i], small_r.at[4, i], peer))
        for i, peer in enumerate(y_peers)
    ]
    for copy in sums_y:
        copy.wait_recv()
    scale = (sum_y[0] + sum_y[1] + sum_y[2] + sum_y[3]) * (1.0 / rows_total)
    factor[...] = scale
    for a in (0, 1):
        for k in range(padded // 128):
            s = slice(k * 128, (k + 1) * 128)
            one = 1.0 / factor[a : a + 1, s]
            inverse[a, s, :] = jnp.broadcast_to(one, (128, 128)).T

    def scaled(a, value, r):
        factor_here = inverse[a, r, :]
        return (value * jnp.concatenate([factor_here, factor_here], axis=1)).astype(BF16)

    def finish(a, along, source, low_ref, h):
        r = slice(h * half, (h + 1) * half)
        if source is None:
            value = latest[a, r, :]
        else:
            value = source[r, :].astype(F32) + lax.dot_general(
                highs[a, :, r], low_ref[...], (((0,), (0,)), ((), ())), preferred_element_type=F32
            )
        first = pl.multiple_of(place(a, along, 0) * width, width)
        out[a][r, pl.ds(first, width)] = scaled(a, value, r)

    hops = {}

    def hop(a, q, along, h):
        for s, d in enumerate(DIRS):
            ref = block(a, along, 0, h * half, half)
            hops[a, s, q, h] = go(
                send(ref, ref, hop_s.at[a, s, q, h], hop_r.at[a, s, q, h], (place(a, 0, d), col))
            )

    for h in (0, 1):
        for a in (0, 1):
            finish(a, 0, None, None, h)
            hop(a, 0, 0, h)

    for copy in raws:
        copy.wait_recv()
    far = {}
    for s, d in enumerate(DIRS):
        for a in (0, 1):
            finish(a, -d, raw.at[a, s], raw_low.at[a, s], s)
            ref = block(a, -d, 0, s * half, half)
            far[a, s] = go(send(ref, ref, far_s.at[a, s], far_r.at[a, s], (place(a, d, 0), col)))
    for s, d in enumerate(DIRS):
        for a in (0, 1):
            finish(a, -d, raw.at[a, s], raw_low.at[a, s], 1 - s)
    for s, d in enumerate(DIRS):
        for h in (0, 1):
            for a in (0, 1):
                hop(a, 1 + s, -d, h)
    for h in (0, 1):
        for a in (0, 1):
            far[a, h].wait_recv()
            hop(a, 3, 2, h)
    for copy in norm_y:
        copy.wait_recv()
    for i in range(stack.shape[1]):
        stack[layer, i : i + 1, :] = norm[0, i] + norm[1, i]

    def to_layer(other):
        return send(stack.at[layer], stack.at[layer], layer_s.at[other], layer_r.at[layer], (zero, 2 * other + core))

    def from_layer(other):
        return send(stack.at[other], stack.at[other], layer_s.at[other], layer_r.at[other], (zero, 2 * other + core))

    for other in range(layers):
        @pl.when(other < layer)
        def _():
            to_layer(other).start()
    def end(a, s, q):
        ref = block(a, ALONG[q], -DIRS[s], s * half, half)
        return send(ref, ref, end_s.at[a, s, q], end_r.at[a, s, q], (place(a, 0, DIRS[s]), col))

    ends = [(a, s, q) for q in range(4) for s in (0, 1) for a in (0, 1)]
    for q in range(4):
        for s in (0, 1):
            for a in (0, 1):
                hops[a, s, q, s].wait_recv()

        @pl.when(jnp.logical_not(is_late(core, q)))
        def _():
            for key in ends:
                if key[2] == q:
                    end(*key).start()
    for other in range(layers):
        @pl.when(other > layer)
        def _():
            from_layer(other).wait_recv()
            to_layer(other).start()
    for other in range(layers):
        @pl.when(other < layer)
        def _():
            from_layer(other).wait_recv()

        @pl.when(other != layer)
        def _():
            to_layer(other).wait_send()
    parts = rows.shape[0] // stack.shape[1]
    for hi in range(parts):
        here = range(hi * layers // parts, (hi + 1) * layers // parts)
        total = sum(stack[k] for k in here)
        for i in range(total.shape[0]):
            rows[parts * i + hi : parts * i + hi + 1, :] = total[i : i + 1, :]
    norm_out[...] = rows[...].astype(BF16)
    for q in range(4):
        for s in (0, 1):
            for a in (0, 1):
                hops[a, s, q, 1 - s].wait_recv()
    for copy in sent:
        copy.wait_send()
    for q in range(4):
        @pl.when(jnp.logical_not(is_late(core, q)))
        def _():
            for key in ends:
                if key[2] == q:
                    end(*key).wait()


def last_relays(out_g, out_u, _, tail, send_sem, recv_sem):
    zero, col = lax.axis_index("zero"), lax.axis_index("cols")
    core = lax.rem(col, 2)
    wide, width = tail.shape[2:]
    half = wide // 2
    barrier = pltpu.get_barrier_semaphore()
    for a in (0, 1):
        for d in DIRS:
            pl.semaphore_signal(barrier, inc=1, device_id=(place_of(a, 0, d), col), device_id_type=MESH)
    pl.semaphore_wait(barrier, 4)

    def end(a, s, q):
        d = DIRS[s]
        first = pl.multiple_of(place_of(a, ALONG[q], -d) * width, width)
        rows = pl.ds(s * half, half)
        return pltpu.make_async_remote_copy(
            src_ref=(out_g, out_u)[a].at[rows, pl.ds(first, width)],
            dst_ref=tail.at[a, q, rows, :],
            send_sem=send_sem.at[a, s, q],
            recv_sem=recv_sem.at[a, s, q],
            device_id=(place_of(a, 0, d), col),
            device_id_type=MESH,
        )

    def each(act):
        for q in range(4):
            @pl.when(is_late(core, q))
            def _():
                for s in (0, 1):
                    for a in (0, 1):
                        act(end(a, s, q))

    each(lambda copy: copy.start())
    each(lambda copy: copy.wait())


def columns(a, along, across, width):
    return pl.ds(pl.multiple_of(place_of(a, along, across) * width, width), width)


def put(width, g, u, factor, norm, out_g, out_u, factor_g, factor_u, norm_out, sem):
    core = lax.rem(lax.axis_index("cols"), 2)

    def copy(a, q, k):
        across = (0, -1, 1, 2)[k]
        here = columns(a, ALONG[q], across, width)
        return pltpu.make_async_copy((g, u)[a].at[:, here], (out_g, out_u)[a].at[:, here], sem.at[a, q, k])

    def each(act):
        for q in range(4):
            for a in (0, 1):
                for k in range(3):
                    act(copy(a, q, k))

            @pl.when(jnp.logical_not(is_late(core, q)))
            def _():
                for a in (0, 1):
                    act(copy(a, q, 3))

    each(lambda c: c.start())
    wide = factor_g.shape[0]
    factor_g[...] = factor[0, :wide]
    factor_u[...] = factor[1, :wide]
    norm_out[...] = norm[...]
    each(lambda c: c.wait())


def put_tail(tail, held_g, held_u, out_g, out_u, sem):
    core = lax.rem(lax.axis_index("cols"), 2)
    width = tail.shape[3]

    def each(act):
        for q in range(4):
            @pl.when(is_late(core, q))
            def _():
                for a in (0, 1):
                    here = columns(a, ALONG[q], 2, width)
                    act(pltpu.make_async_copy(tail.at[a, q], (out_g, out_u)[a].at[:, here], sem.at[a, q]))

    each(lambda c: c.start())
    each(lambda c: c.wait())


def shards(devices, cols, train_gate, low_gate, high_gate, train_up, low_up, high_up, norm_train, norm_step):
    width, wide = train_gate.shape
    rank = low_gate.shape[1]
    padded = -(-wide // 128) * 128
    rows_total = width * devices
    gain = norm_train.shape[0]
    layers = cols // 2
    rows = devices * cols * gain // 128
    hbm = pl.BlockSpec(memory_space=pltpu.HBM)
    vmem = pl.BlockSpec(memory_space=pltpu.VMEM)
    dma = pltpu.SemaphoreType.DMA
    out_g, out_u, factor, norm = pl.pallas_call(
        functools.partial(kernel, layers, rows_total),
        out_shape=(
            pltpu.VMEM((wide, rows_total), BF16),
            pltpu.VMEM((wide, rows_total), BF16),
            jax.ShapeDtypeStruct((2, padded), F32),
            jax.ShapeDtypeStruct((rows, 128), BF16),
        ),
        in_specs=[hbm] * 8,
        out_specs=[vmem] * 4,
        scratch_shapes=[
            pltpu.VMEM((2, devices, 1, 128), F32),
            pltpu.VMEM((layers, devices, 128), F32),
            pltpu.VMEM((rows, 128), F32),
            pltpu.VMEM((2, 1, gain), F32),
            pltpu.VMEM((2, wide, width), BF16),
            pltpu.VMEM((2, rank, width), BF16),
            pltpu.VMEM((2, rank, wide), BF16),
            pltpu.VMEM((2, 2, wide, width), BF16),
            pltpu.VMEM((2, 2, rank, width), BF16),
            pltpu.VMEM((2, wide, width), F32),
            pltpu.VMEM((2, padded, width // 2), F32),
            pltpu.VMEM((2, padded, 128), F32),
            pltpu.VMEM((SIDE, 2, padded), F32),
            pltpu.VMEM((SIDE, 2, padded), F32),
            dma((2,)), dma((2, 3)),
            dma((2, 2, 4)), dma((2, 2, 4)),
            dma((2, 2)), dma((2, 2)),
            dma((2, 2)), dma((2, 2)),
            dma((2, 2, 4, 2)), dma((2, 2, 4, 2)),
            dma((2, 2, 4)), dma((2, 2, 4)),
            dma((5, 3)), dma((5, 3)),
            dma((layers,)), dma((layers,)),
        ],
        compiler_params=pltpu.CompilerParams(
            collective_id=0, has_side_effects=True, vmem_limit_bytes=24 * 1024 * 1024
        ),
    )(
        *(
            pltpu.with_memory_space_constraint(array, pltpu.HBM)
            for array in (
                train_gate.T, train_up.T, low_gate.T, low_up.T, high_gate, high_up,
                norm_train.reshape(1, -1), norm_step.reshape(1, -1),
            )
        )
    )
    whole = jax.ShapeDtypeStruct((wide, rows_total), BF16)
    ready_g, ready_u, factor_g, factor_u, norm = pl.pallas_call(
        functools.partial(put, width),
        out_shape=(
            whole,
            whole,
            jax.ShapeDtypeStruct((wide,), F32),
            jax.ShapeDtypeStruct((wide,), F32),
            jax.ShapeDtypeStruct((rows, 128), BF16),
        ),
        in_specs=[vmem] * 4,
        out_specs=[hbm] * 2 + [vmem] * 3,
        scratch_shapes=[dma((2, 4, 4))],
        compiler_params=pltpu.CompilerParams(vmem_limit_bytes=1024 * 1024),
    )(out_g, out_u, factor, norm)
    tail = pl.pallas_call(
        last_relays,
        out_shape=pltpu.VMEM((2, 4, wide, width), BF16),
        in_specs=[vmem] * 2 + [hbm],
        out_specs=vmem,
        scratch_shapes=[dma((2, 2, 4)), dma((2, 2, 4))],
        compiler_params=pltpu.CompilerParams(
            collective_id=1, has_side_effects=True, vmem_limit_bytes=1024 * 1024
        ),
    )(out_g, out_u, pltpu.with_memory_space_constraint(norm, pltpu.HBM))
    ready_g, ready_u = pl.pallas_call(
        put_tail,
        out_shape=(whole, whole),
        in_specs=[vmem, hbm, hbm],
        out_specs=[hbm] * 2,
        input_output_aliases={1: 0, 2: 1},
        scratch_shapes=[dma((2, 4))],
        compiler_params=pltpu.CompilerParams(vmem_limit_bytes=1024 * 1024),
    )(tail, ready_g, ready_u)
    return ready_g.T, ready_u.T, factor_g, factor_u, norm.reshape(-1)


def solution(mesh):
    return jax.shard_map(
        functools.partial(shards, mesh.shape["zero"], mesh.shape["cols"]),
        mesh=mesh,
        in_specs=(
            P("zero", "cols"),
            P("zero", None),
            P(None, "cols"),
            P("zero", "cols"),
            P("zero", None),
            P(None, "cols"),
            P(("zero", "cols")),
            P(("zero", "cols")),
        ),
        out_specs=(P(None, "cols"), P(None, "cols"), P("cols"), P("cols"), P()),
        check_vma=False,
    )
```

```python
import functools

import jax
import jax.numpy as jnp
from jax import lax
from jax.experimental import pallas as pl
from jax.experimental.pallas import tpu as pltpu
from jax.sharding import PartitionSpec as P

MESH = pl.DeviceIdType.MESH
F32 = jnp.float32
BF16 = jnp.bfloat16
SIDE = 4
DIRS = (1, -1)
ALONG = (0, -1, 1, 2)


def wrap(i, n):
    return lax.rem(i + n, n)


def is_late(core, q):
    return jnp.logical_or(core == 1, q == 3)


def place_of(a, along, across):
    zero = lax.axis_index("zero")
    dx, dy = (along, across) if a == 0 else (across, along)
    return wrap(lax.div(zero, SIDE) + dy, SIDE) * SIDE + wrap(lax.rem(zero, SIDE) + dx, SIDE)


def kernel(
    layers,
    rows_total,
    train_g, train_u, low_g, low_u, high_g, high_u, norm_a, norm_b,
    out_g, out_u, factor, norm_out,
    norm, stack, rows, gains, own, lows, highs, raw, raw_low, latest, part, inverse, sum_x, sum_y,
    gain_sem, in_sem, raw_s, raw_r, low_s, low_r, far_s, far_r, hop_s, hop_r, end_s, end_r, small_s, small_r, layer_s, layer_r,
):
    wide, width = own.shape[1:]
    half = wide // 2
    cut = half // 2 // 16 * 16
    pieces = ((0, cut), (cut, half - cut), (half, cut), (half + cut, half - cut))
    zero, col = lax.axis_index("zero"), lax.axis_index("cols")
    x, y = lax.rem(zero, SIDE), lax.div(zero, SIDE)
    train, low, high, out = (train_g, train_u), (low_g, low_u), (high_g, high_u), (out_g, out_u)

    place = place_of

    def block(a, q, k, start, size, count=1):
        return out[a].at[pl.ds(start, size), pl.ds((k * SIDE + q) * width, count * width)]

    def send(src, dst, ssem, rsem, to):
        return pltpu.make_async_remote_copy(
            src_ref=src, dst_ref=dst, send_sem=ssem, recv_sem=rsem, device_id=to, device_id_type=MESH
        )

    x_peers = [(y * SIDE + wrap(x + o, SIDE), col) for o in range(1, SIDE)]
    y_peers = [(wrap(y + o, SIDE) * SIDE + x, col) for o in range(1, SIDE)]
    c_peers = [(zero, col + 1 - 2 * lax.rem(col, 2))]

    barrier = pltpu.get_barrier_semaphore()
    for peer in x_peers + y_peers + c_peers:
        pl.semaphore_signal(barrier, inc=1, device_id=peer, device_id_type=MESH)

    gain_loads = [pltpu.make_async_copy(n, gains.at[i], gain_sem.at[i]) for i, n in enumerate((norm_a, norm_b))]
    for load in gain_loads:
        load.start()
    core, layer = lax.rem(col, 2), lax.div(col, 2)
    for other in range(1, layers):
        @pl.when(other > layer)
        def _():
            pl.semaphore_signal(barrier, inc=1, device_id=(zero, 2 * other + core), device_id_type=MESH)

    loads = []
    for a in (0, 1):
        loads.append(pltpu.make_async_copy(train[a], own.at[a], in_sem.at[a, 0]))
        loads.append(pltpu.make_async_copy(low[a], lows.at[a], in_sem.at[a, 1]))
        loads.append(pltpu.make_async_copy(high[a], highs.at[a], in_sem.at[a, 2]))
    for load in loads:
        load.start()

    for load in gain_loads:
        load.wait()
    value = gains[0] + gains[1]
    spread = jnp.concatenate([value] * (128 // value.shape[1]), axis=1)
    group = lax.broadcasted_iota(jnp.int32, (1, 128), 1) // value.shape[1]
    mine = lax.rem(col, 128 // value.shape[1])
    norm[core, zero] = jnp.where(group == mine, spread, jnp.zeros_like(spread))
    pl.semaphore_wait(barrier, len(x_peers) + len(y_peers) + len(c_peers) + layer)

    sent = []

    def go(copy):
        copy.start()
        sent.append(copy)
        return copy

    def send_raw(p):
        start, size = pieces[p]
        return [
            go(send(train[a].at[pl.ds(start, size), :], raw.at[a, s, pl.ds(start, size), :],
                    raw_s.at[a, s, p], raw_r.at[a, s, p], (place(a, d, 0), col)))
            for a in (0, 1) for s, d in enumerate(DIRS)
        ]

    raws = send_raw(0)
    raws += [
        go(send(low[a], raw_low.at[a, s], low_s.at[a, s], low_r.at[a, s], (place(a, d, 0), col)))
        for a in (0, 1) for s, d in enumerate(DIRS)
    ]
    norm_c = [
        go(send(norm.at[core, zero], norm.at[core, zero], small_s.at[0, i], small_r.at[0, i], peer))
        for i, peer in enumerate(c_peers)
    ]
    for load in loads:
        load.wait()

    padded = part.shape[1]
    for a in (0, 1):
        if padded > wide:
            part[a, wide:, :] = jnp.zeros((padded - wide, part.shape[2]), F32)
        for h in (0, 1):
            r = slice(h * half, (h + 1) * half)
            fresh = own[a, r, :].astype(F32) + lax.dot_general(
                highs[a, :, r], lows[a], (((0,), (0,)), ((), ())), preferred_element_type=F32
            )
            latest[a, r, :] = fresh
            size = jnp.abs(fresh)
            part[a, r, :] = size[:, : width // 2] + size[:, width // 2 :]
        for k in range(padded // 128):
            s = slice(k * 128, (k + 1) * 128)
            sum_x[x, a : a + 1, s] = jnp.sum(part[a, s, :].T, axis=0, keepdims=True)

    sums_x = [
        go(send(sum_x.at[x], sum_x.at[x], small_s.at[1, i], small_r.at[1, i], peer))
        for i, peer in enumerate(x_peers)
    ]
    raws += send_raw(1)
    for copy in norm_c:
        copy.wait_recv()
    norm_x = [
        go(send(norm.at[:, zero], norm.at[:, zero], small_s.at[2, i], small_r.at[2, i], peer))
        for i, peer in enumerate(x_peers)
    ]
    for copy in sums_x:
        copy.wait_recv()
    sum_y[y] = sum_x[0] + sum_x[1] + sum_x[2] + sum_x[3]
    sums_y = [
        go(send(sum_y.at[y], sum_y.at[y], small_s.at[3, i], small_r.at[3, i], peer))
        for i, peer in enumerate(y_peers)
    ]
    raws += send_raw(2)
    raws += send_raw(3)
    for copy in norm_x:
        copy.wait_recv()
    row = pl.ds(y * SIDE, SIDE)
    norm_y = [
        go(send(norm.at[:, row], norm.at[:, row], small_s.at[4, i], small_r.at[4, i], peer))
        for i, peer in enumerate(y_peers)
    ]
    for copy in sums_y:
        copy.wait_recv()
    scale = (sum_y[0] + sum_y[1] + sum_y[2] + sum_y[3]) * (1.0 / rows_total)
    factor[...] = scale
    for a in (0, 1):
        for k in range(padded // 128):
            s = slice(k * 128, (k + 1) * 128)
            one = 1.0 / factor[a : a + 1, s]
            inverse[a, s, :] = jnp.broadcast_to(one, (128, 128)).T

    def scaled(a, value, r):
        factor_here = inverse[a, r, :]
        return (value * jnp.concatenate([factor_here, factor_here], axis=1)).astype(BF16)

    def finish(a, q, source, low_ref, h):
        r = slice(h * half, (h + 1) * half)
        if source is None:
            value = latest[a, r, :]
        else:
            value = source[r, :].astype(F32) + lax.dot_general(
                highs[a, :, r], low_ref[...], (((0,), (0,)), ((), ())), preferred_element_type=F32
            )
        out[a][r, q * width : (q + 1) * width] = scaled(a, value, r)

    hops = {}

    def hop(a, g):
        q, count = ((0, 1), (1, 2), (3, 1))[g]
        for s, d in enumerate(DIRS):
            hops[a, s, g] = go(
                send(block(a, q, 0, 0, wide, count), block(a, q, 1 + s, 0, wide, count),
                     hop_s.at[a, s, g], hop_r.at[a, s, g], (place(a, 0, d), col))
            )

    for a in (0, 1):
        for h in (0, 1):
            finish(a, 0, None, None, h)
        hop(a, 0)

    for copy in raws:
        copy.wait_recv()
    far = []
    for s, d in enumerate(DIRS):
        for a in (0, 1):
            finish(a, 1 + s, raw.at[a, s], raw_low.at[a, s], s)
            far.append(go(
                send(block(a, 1 + s, 0, s * half, half), block(a, 3, 0, s * half, half),
                     far_s.at[a, s], far_r.at[a, s], (place(a, d, 0), col))
            ))
    for a in (0, 1):
        for s in (0, 1):
            finish(a, 1 + s, raw.at[a, s], raw_low.at[a, s], 1 - s)
        hop(a, 1)
    for copy in far:
        copy.wait_recv()
    for a in (0, 1):
        hop(a, 2)
    for copy in norm_y:
        copy.wait_recv()
    for i in range(stack.shape[1]):
        stack[layer, i : i + 1, :] = norm[0, i] + norm[1, i]

    def to_layer(other):
        return send(stack.at[layer], stack.at[layer], layer_s.at[other], layer_r.at[layer], (zero, 2 * other + core))

    def from_layer(other):
        return send(stack.at[other], stack.at[other], layer_s.at[other], layer_r.at[other], (zero, 2 * other + core))

    for other in range(layers):
        @pl.when(other < layer)
        def _():
            to_layer(other).start()
    ends = [
        send(block(a, 0, 1 + s, s * half, half, 3), block(a, 0, 3, s * half, half, 3),
             end_s.at[a, s], end_r.at[a, s], (place(a, 0, d), col))
        for s, d in enumerate(DIRS) for a in (0, 1)
    ]
    for g in range(2):
        for s in (0, 1):
            for a in (0, 1):
                hops[a, s, g].wait_recv()

    @pl.when(core == 0)
    def _():
        for copy in ends:
            copy.start()

    for other in range(layers):
        @pl.when(other > layer)
        def _():
            from_layer(other).wait_recv()
            to_layer(other).start()
    for other in range(layers):
        @pl.when(other < layer)
        def _():
            from_layer(other).wait_recv()

        @pl.when(other != layer)
        def _():
            to_layer(other).wait_send()
    parts = rows.shape[0] // stack.shape[1]
    for hi in range(parts):
        here = range(hi * layers // parts, (hi + 1) * layers // parts)
        total = sum(stack[k] for k in here)
        for i in range(total.shape[0]):
            rows[parts * i + hi : parts * i + hi + 1, :] = total[i : i + 1, :]
    norm_out[...] = rows[...].astype(BF16)
    for s in (0, 1):
        for a in (0, 1):
            hops[a, s, 2].wait_recv()
    for copy in sent:
        copy.wait_send()

    @pl.when(core == 0)
    def _():
        for copy in ends:
            copy.wait()


def last_relays(out_g, out_u, _, tail, send_sem, recv_sem):
    zero, col = lax.axis_index("zero"), lax.axis_index("cols")
    core = lax.rem(col, 2)
    wide, width = tail.shape[1], tail.shape[2] // SIDE
    half = wide // 2
    barrier = pltpu.get_barrier_semaphore()
    for a in (0, 1):
        for d in DIRS:
            pl.semaphore_signal(barrier, inc=1, device_id=(place_of(a, 0, d), col), device_id_type=MESH)
    pl.semaphore_wait(barrier, 4)

    def relay(q):
        copies = [
            pltpu.make_async_remote_copy(
                src_ref=(out_g, out_u)[a].at[rows, pl.ds(((1 + s) * SIDE + q) * width, (SIDE - q) * width)],
                dst_ref=tail.at[a, rows, pl.ds(q * width, (SIDE - q) * width)],
                send_sem=send_sem.at[a, s],
                recv_sem=recv_sem.at[a, s],
                device_id=(place_of(a, 0, d), col),
                device_id_type=MESH,
            )
            for s, d in enumerate(DIRS) for a in (0, 1) for rows in (pl.ds(s * half, half),)
        ]
        for copy in copies:
            copy.start()
        for copy in copies:
            copy.wait()

    @pl.when(core == 0)
    def _():
        relay(3)

    @pl.when(core == 1)
    def _():
        relay(0)


def columns(a, along, across, width):
    return pl.ds(pl.multiple_of(place_of(a, along, across) * width, width), width)


def put(width, g, u, factor, norm, out_g, out_u, factor_g, factor_u, norm_out, sem):
    core = lax.rem(lax.axis_index("cols"), 2)

    def copy(a, q, k):
        held = pl.ds((k * SIDE + q) * width, width)
        here = columns(a, ALONG[q], ALONG[k], width)
        return pltpu.make_async_copy((g, u)[a].at[:, held], (out_g, out_u)[a].at[:, here], sem.at[a, q, k])

    def each(act):
        for q in range(4):
            for a in (0, 1):
                for k in range(3):
                    act(copy(a, q, k))

            @pl.when(jnp.logical_not(is_late(core, q)))
            def _():
                for a in (0, 1):
                    act(copy(a, q, 3))

    each(lambda c: c.start())
    wide = factor_g.shape[0]
    factor_g[...] = factor[0, :wide]
    factor_u[...] = factor[1, :wide]
    norm_out[...] = norm[...]
    each(lambda c: c.wait())


def put_tail(tail, held_g, held_u, out_g, out_u, sem):
    core = lax.rem(lax.axis_index("cols"), 2)
    width = tail.shape[2] // SIDE

    def each(act):
        for q in range(4):
            @pl.when(is_late(core, q))
            def _():
                for a in (0, 1):
                    here = columns(a, ALONG[q], 2, width)
                    act(pltpu.make_async_copy(tail.at[a, :, pl.ds(q * width, width)], (out_g, out_u)[a].at[:, here], sem.at[a, q]))

    each(lambda c: c.start())
    each(lambda c: c.wait())


def shards(devices, cols, train_gate, low_gate, high_gate, train_up, low_up, high_up, norm_train, norm_step):
    width, wide = train_gate.shape
    rank = low_gate.shape[1]
    padded = -(-wide // 128) * 128
    rows_total = width * devices
    gain = norm_train.shape[0]
    layers = cols // 2
    rows = devices * cols * gain // 128
    hbm = pl.BlockSpec(memory_space=pltpu.HBM)
    vmem = pl.BlockSpec(memory_space=pltpu.VMEM)
    dma = pltpu.SemaphoreType.DMA
    out_g, out_u, factor, norm = pl.pallas_call(
        functools.partial(kernel, layers, rows_total),
        out_shape=(
            pltpu.VMEM((wide, rows_total), BF16),
            pltpu.VMEM((wide, rows_total), BF16),
            jax.ShapeDtypeStruct((2, padded), F32),
            jax.ShapeDtypeStruct((rows, 128), BF16),
        ),
        in_specs=[hbm] * 8,
        out_specs=[vmem] * 4,
        scratch_shapes=[
            pltpu.VMEM((2, devices, 1, 128), F32),
            pltpu.VMEM((layers, devices, 128), F32),
            pltpu.VMEM((rows, 128), F32),
            pltpu.VMEM((2, 1, gain), F32),
            pltpu.VMEM((2, wide, width), BF16),
            pltpu.VMEM((2, rank, width), BF16),
            pltpu.VMEM((2, rank, wide), BF16),
            pltpu.VMEM((2, 2, wide, width), BF16),
            pltpu.VMEM((2, 2, rank, width), BF16),
            pltpu.VMEM((2, wide, width), F32),
            pltpu.VMEM((2, padded, width // 2), F32),
            pltpu.VMEM((2, padded, 128), F32),
            pltpu.VMEM((SIDE, 2, padded), F32),
            pltpu.VMEM((SIDE, 2, padded), F32),
            dma((2,)), dma((2, 3)),
            dma((2, 2, 4)), dma((2, 2, 4)),
            dma((2, 2)), dma((2, 2)),
            dma((2, 2)), dma((2, 2)),
            dma((2, 2, 3)), dma((2, 2, 3)),
            dma((2, 2)), dma((2, 2)),
            dma((5, 3)), dma((5, 3)),
            dma((layers,)), dma((layers,)),
        ],
        compiler_params=pltpu.CompilerParams(
            collective_id=0, has_side_effects=True, vmem_limit_bytes=24 * 1024 * 1024
        ),
    )(
        *(
            pltpu.with_memory_space_constraint(array, pltpu.HBM)
            for array in (
                train_gate.T, train_up.T, low_gate.T, low_up.T, high_gate, high_up,
                norm_train.reshape(1, -1), norm_step.reshape(1, -1),
            )
        )
    )
    whole = jax.ShapeDtypeStruct((wide, rows_total), BF16)
    ready_g, ready_u, factor_g, factor_u, norm = pl.pallas_call(
        functools.partial(put, width),
        out_shape=(
            whole,
            whole,
            jax.ShapeDtypeStruct((wide,), F32),
            jax.ShapeDtypeStruct((wide,), F32),
            jax.ShapeDtypeStruct((rows, 128), BF16),
        ),
        in_specs=[vmem] * 4,
        out_specs=[hbm] * 2 + [vmem] * 3,
        scratch_shapes=[dma((2, 4, 4))],
        compiler_params=pltpu.CompilerParams(vmem_limit_bytes=1024 * 1024),
    )(out_g, out_u, factor, norm)
    tail = pl.pallas_call(
        last_relays,
        out_shape=pltpu.VMEM((2, wide, SIDE * width), BF16),
        in_specs=[vmem] * 2 + [hbm],
        out_specs=vmem,
        scratch_shapes=[dma((2, 2)), dma((2, 2))],
        compiler_params=pltpu.CompilerParams(
            collective_id=1, has_side_effects=True, vmem_limit_bytes=1024 * 1024
        ),
    )(out_g, out_u, pltpu.with_memory_space_constraint(norm, pltpu.HBM))
    ready_g, ready_u = pl.pallas_call(
        put_tail,
        out_shape=(whole, whole),
        in_specs=[vmem, hbm, hbm],
        out_specs=[hbm] * 2,
        input_output_aliases={1: 0, 2: 1},
        scratch_shapes=[dma((2, 4))],
        compiler_params=pltpu.CompilerParams(vmem_limit_bytes=1024 * 1024),
    )(tail, ready_g, ready_u)
    return ready_g.T, ready_u.T, factor_g, factor_u, norm.reshape(-1)


def solution(mesh):
    return jax.shard_map(
        functools.partial(shards, mesh.shape["zero"], mesh.shape["cols"]),
        mesh=mesh,
        in_specs=(
            P("zero", "cols"),
            P("zero", None),
            P(None, "cols"),
            P("zero", "cols"),
            P("zero", None),
            P(None, "cols"),
            P(("zero", "cols")),
            P(("zero", "cols")),
        ),
        out_specs=(P(None, "cols"), P(None, "cols"), P("cols"), P("cols"), P()),
        check_vma=False,
    )
```

```python
import functools

import jax
import jax.numpy as jnp
from jax import lax
from jax.experimental import pallas as pl
from jax.experimental.pallas import tpu as pltpu
from jax.sharding import PartitionSpec as P

MESH = pl.DeviceIdType.MESH
F32 = jnp.float32
BF16 = jnp.bfloat16
SIDE = 4
DIRS = (1, -1)
ALONG = (0, -1, 1, 2)


def wrap(i, n):
    return lax.rem(i + n, n)


def is_late(core, q):
    return jnp.logical_or(core == 1, q == 3)


def place_of(a, along, across):
    zero = lax.axis_index("zero")
    dx, dy = (along, across) if a == 0 else (across, along)
    return wrap(lax.div(zero, SIDE) + dy, SIDE) * SIDE + wrap(lax.rem(zero, SIDE) + dx, SIDE)


def kernel(
    layers,
    rows_total,
    train_g, train_u, low_g, low_u, high_g, high_u, norm_a, norm_b,
    out_g, out_u, factor, norm_out,
    norm, stack, rows, gains, own, lows, highs, raw, raw_low, latest, part, inverse, sum_x, sum_y,
    gain_sem, in_sem, raw_s, raw_r, low_s, low_r, far_s, far_r, hop_s, hop_r, end_s, end_r, small_s, small_r, layer_s, layer_r,
):
    wide, width = own.shape[1:]
    half = wide // 2
    cuts = [0] + [wide * part // 16 // 16 * 16 for part in (6, 10, 13)] + [wide]
    pieces = [(lo, hi - lo) for lo, hi in zip(cuts, cuts[1:])]
    zero, col = lax.axis_index("zero"), lax.axis_index("cols")
    x, y = lax.rem(zero, SIDE), lax.div(zero, SIDE)
    train, low, high, out = (train_g, train_u), (low_g, low_u), (high_g, high_u), (out_g, out_u)

    place = place_of

    def block(a, q, k, start, size, count=1):
        return out[a].at[pl.ds(start, size), pl.ds((k * SIDE + q) * width, count * width)]

    def send(src, dst, ssem, rsem, to):
        return pltpu.make_async_remote_copy(
            src_ref=src, dst_ref=dst, send_sem=ssem, recv_sem=rsem, device_id=to, device_id_type=MESH
        )

    x_peers = [(y * SIDE + wrap(x + o, SIDE), col) for o in range(1, SIDE)]
    y_peers = [(wrap(y + o, SIDE) * SIDE + x, col) for o in range(1, SIDE)]
    c_peers = [(zero, col + 1 - 2 * lax.rem(col, 2))]

    barrier = pltpu.get_barrier_semaphore()
    for peer in x_peers + y_peers + c_peers:
        pl.semaphore_signal(barrier, inc=1, device_id=peer, device_id_type=MESH)

    gain_loads = [pltpu.make_async_copy(n, gains.at[i], gain_sem.at[i]) for i, n in enumerate((norm_a, norm_b))]
    for load in gain_loads:
        load.start()
    core, layer = lax.rem(col, 2), lax.div(col, 2)
    for other in range(1, layers):
        @pl.when(other > layer)
        def _():
            pl.semaphore_signal(barrier, inc=1, device_id=(zero, 2 * other + core), device_id_type=MESH)

    loads = []
    for a in (0, 1):
        loads.append(pltpu.make_async_copy(train[a], own.at[a], in_sem.at[a, 0]))
        loads.append(pltpu.make_async_copy(low[a], lows.at[a], in_sem.at[a, 1]))
        loads.append(pltpu.make_async_copy(high[a], highs.at[a], in_sem.at[a, 2]))
    for load in loads:
        load.start()

    pl.semaphore_wait(barrier, len(x_peers) + len(y_peers) + len(c_peers) + layer)

    sent = []

    def go(copy):
        copy.start()
        sent.append(copy)
        return copy

    def send_raw(p):
        start, size = pieces[p]
        return [
            go(send(train[a].at[pl.ds(start, size), :], raw.at[a, s, pl.ds(start, size), :],
                    raw_s.at[a, s, p], raw_r.at[a, s, p], (place(a, d, 0), col)))
            for a in (0, 1) for s, d in enumerate(DIRS)
        ]

    raws = send_raw(0)
    raws += [
        go(send(low[a], raw_low.at[a, s], low_s.at[a, s], low_r.at[a, s], (place(a, d, 0), col)))
        for a in (0, 1) for s, d in enumerate(DIRS)
    ]
    for load in gain_loads:
        load.wait()
    value = gains[0] + gains[1]
    spread = jnp.concatenate([value] * (128 // value.shape[1]), axis=1)
    group = lax.broadcasted_iota(jnp.int32, (1, 128), 1) // value.shape[1]
    mine = lax.rem(col, 128 // value.shape[1])
    norm[core, zero] = jnp.where(group == mine, spread, jnp.zeros_like(spread))
    norm_c = [
        go(send(norm.at[core, zero], norm.at[core, zero], small_s.at[0, i], small_r.at[0, i], peer))
        for i, peer in enumerate(c_peers)
    ]
    for load in loads:
        load.wait()

    padded = part.shape[1]
    for a in (0, 1):
        if padded > wide:
            part[a, wide:, :] = jnp.zeros((padded - wide, part.shape[2]), F32)
        for h in (0, 1):
            r = slice(h * half, (h + 1) * half)
            fresh = own[a, r, :].astype(F32) + lax.dot_general(
                highs[a, :, r], lows[a], (((0,), (0,)), ((), ())), preferred_element_type=F32
            )
            latest[a, r, :] = fresh
            size = jnp.abs(fresh)
            part[a, r, :] = size[:, : width // 2] + size[:, width // 2 :]
        for k in range(padded // 128):
            s = slice(k * 128, (k + 1) * 128)
            sum_x[x, a : a + 1, s] = jnp.sum(part[a, s, :].T, axis=0, keepdims=True)

    sums_x = [
        go(send(sum_x.at[x], sum_x.at[x], small_s.at[1, i], small_r.at[1, i], peer))
        for i, peer in enumerate(x_peers)
    ]
    raws += send_raw(1)
    for copy in norm_c:
        copy.wait_recv()
    norm_x = [
        go(send(norm.at[:, zero], norm.at[:, zero], small_s.at[2, i], small_r.at[2, i], peer))
        for i, peer in enumerate(x_peers)
    ]
    for copy in sums_x:
        copy.wait_recv()
    sum_y[y] = sum_x[0] + sum_x[1] + sum_x[2] + sum_x[3]
    sums_y = [
        go(send(sum_y.at[y], sum_y.at[y], small_s.at[3, i], small_r.at[3, i], peer))
        for i, peer in enumerate(y_peers)
    ]
    raws += send_raw(2)
    raws += send_raw(3)
    for copy in norm_x:
        copy.wait_recv()
    row = pl.ds(y * SIDE, SIDE)
    norm_y = [
        go(send(norm.at[:, row], norm.at[:, row], small_s.at[4, i], small_r.at[4, i], peer))
        for i, peer in enumerate(y_peers)
    ]
    for copy in sums_y:
        copy.wait_recv()
    scale = (sum_y[0] + sum_y[1] + sum_y[2] + sum_y[3]) * (1.0 / rows_total)
    factor[...] = scale
    for a in (0, 1):
        for k in range(padded // 128):
            s = slice(k * 128, (k + 1) * 128)
            one = 1.0 / factor[a : a + 1, s]
            inverse[a, s, :] = jnp.broadcast_to(one, (128, 128)).T

    def scaled(a, value, r):
        factor_here = inverse[a, r, :]
        return (value * jnp.concatenate([factor_here, factor_here], axis=1)).astype(BF16)

    def finish(a, q, source, low_ref, h):
        r = slice(h * half, (h + 1) * half)
        if source is None:
            value = latest[a, r, :]
        else:
            value = source[r, :].astype(F32) + lax.dot_general(
                highs[a, :, r], low_ref[...], (((0,), (0,)), ((), ())), preferred_element_type=F32
            )
        out[a][r, q * width : (q + 1) * width] = scaled(a, value, r)

    hops = {}

    def hop(a, g):
        q, count = ((0, 1), (1, 2), (3, 1))[g]
        for s, d in enumerate(DIRS):
            hops[a, s, g] = go(
                send(block(a, q, 0, 0, wide, count), block(a, q, 1 + s, 0, wide, count),
                     hop_s.at[a, s, g], hop_r.at[a, s, g], (place(a, 0, d), col))
            )

    for a in (0, 1):
        for h in (0, 1):
            finish(a, 0, None, None, h)
        hop(a, 0)

    for copy in raws:
        copy.wait_recv()
    far = []
    for s, d in enumerate(DIRS):
        for a in (0, 1):
            finish(a, 1 + s, raw.at[a, s], raw_low.at[a, s], s)
            far.append(go(
                send(block(a, 1 + s, 0, s * half, half), block(a, 3, 0, s * half, half),
                     far_s.at[a, s], far_r.at[a, s], (place(a, d, 0), col))
            ))
    for a in (0, 1):
        for s in (0, 1):
            finish(a, 1 + s, raw.at[a, s], raw_low.at[a, s], 1 - s)
        hop(a, 1)
    for copy in far:
        copy.wait_recv()
    for a in (0, 1):
        hop(a, 2)
    for copy in norm_y:
        copy.wait_recv()
    for i in range(stack.shape[1]):
        stack[layer, i : i + 1, :] = norm[0, i] + norm[1, i]

    def to_layer(other):
        return send(stack.at[layer], stack.at[layer], layer_s.at[other], layer_r.at[layer], (zero, 2 * other + core))

    def from_layer(other):
        return send(stack.at[other], stack.at[other], layer_s.at[other], layer_r.at[other], (zero, 2 * other + core))

    for other in range(layers):
        @pl.when(other < layer)
        def _():
            to_layer(other).start()
    ends = [
        send(block(a, 0, 1 + s, s * half, half, 3), block(a, 0, 3, s * half, half, 3),
             end_s.at[a, s], end_r.at[a, s], (place(a, 0, d), col))
        for s, d in enumerate(DIRS) for a in (0, 1)
    ]
    for g in range(2):
        for s in (0, 1):
            for a in (0, 1):
                hops[a, s, g].wait_recv()

    @pl.when(core == 0)
    def _():
        for copy in ends:
            copy.start()

    for other in range(layers):
        @pl.when(other > layer)
        def _():
            from_layer(other).wait_recv()
            to_layer(other).start()
    for other in range(layers):
        @pl.when(other < layer)
        def _():
            from_layer(other).wait_recv()

        @pl.when(other != layer)
        def _():
            to_layer(other).wait_send()
    parts = rows.shape[0] // stack.shape[1]
    for hi in range(parts):
        here = range(hi * layers // parts, (hi + 1) * layers // parts)
        total = sum(stack[k] for k in here)
        for i in range(total.shape[0]):
            rows[parts * i + hi : parts * i + hi + 1, :] = total[i : i + 1, :]
    norm_out[...] = rows[...].astype(BF16)
    for s in (0, 1):
        for a in (0, 1):
            hops[a, s, 2].wait_recv()
    for copy in sent:
        copy.wait_send()

    @pl.when(core == 0)
    def _():
        for copy in ends:
            copy.wait()


def last_relays(out_g, out_u, _, tail, send_sem, recv_sem):
    zero, col = lax.axis_index("zero"), lax.axis_index("cols")
    core = lax.rem(col, 2)
    wide, width = tail.shape[1], tail.shape[2] // SIDE
    half = wide // 2
    barrier = pltpu.get_barrier_semaphore()
    for a in (0, 1):
        for d in DIRS:
            pl.semaphore_signal(barrier, inc=1, device_id=(place_of(a, 0, d), col), device_id_type=MESH)
    pl.semaphore_wait(barrier, 4)

    def relay(q):
        copies = [
            pltpu.make_async_remote_copy(
                src_ref=(out_g, out_u)[a].at[rows, pl.ds(((1 + s) * SIDE + q) * width, (SIDE - q) * width)],
                dst_ref=tail.at[a, rows, pl.ds(q * width, (SIDE - q) * width)],
                send_sem=send_sem.at[a, s],
                recv_sem=recv_sem.at[a, s],
                device_id=(place_of(a, 0, d), col),
                device_id_type=MESH,
            )
            for s, d in enumerate(DIRS) for a in (0, 1) for rows in (pl.ds(s * half, half),)
        ]
        for copy in copies:
            copy.start()
        for copy in copies:
            copy.wait()

    @pl.when(core == 0)
    def _():
        relay(3)

    @pl.when(core == 1)
    def _():
        relay(0)


def columns(a, along, across, width):
    return pl.ds(pl.multiple_of(place_of(a, along, across) * width, width), width)


def put(width, g, u, factor, norm, out_g, out_u, factor_g, factor_u, norm_out, sem):
    core = lax.rem(lax.axis_index("cols"), 2)

    def copy(a, q, k):
        held = pl.ds((k * SIDE + q) * width, width)
        here = columns(a, ALONG[q], ALONG[k], width)
        return pltpu.make_async_copy((g, u)[a].at[:, held], (out_g, out_u)[a].at[:, here], sem.at[a, q, k])

    def each(act):
        for q in range(4):
            for a in (0, 1):
                for k in range(3):
                    act(copy(a, q, k))

            @pl.when(jnp.logical_not(is_late(core, q)))
            def _():
                for a in (0, 1):
                    act(copy(a, q, 3))

    each(lambda c: c.start())
    wide = factor_g.shape[0]
    factor_g[...] = factor[0, :wide]
    factor_u[...] = factor[1, :wide]
    norm_out[...] = norm[...]
    each(lambda c: c.wait())


def put_tail(tail, held_g, held_u, out_g, out_u, sem):
    core = lax.rem(lax.axis_index("cols"), 2)
    width = tail.shape[2] // SIDE

    def each(act):
        for q in range(4):
            @pl.when(is_late(core, q))
            def _():
                for a in (0, 1):
                    here = columns(a, ALONG[q], 2, width)
                    act(pltpu.make_async_copy(tail.at[a, :, pl.ds(q * width, width)], (out_g, out_u)[a].at[:, here], sem.at[a, q]))

    each(lambda c: c.start())
    each(lambda c: c.wait())


def shards(devices, cols, train_gate, low_gate, high_gate, train_up, low_up, high_up, norm_train, norm_step):
    width, wide = train_gate.shape
    rank = low_gate.shape[1]
    padded = -(-wide // 128) * 128
    rows_total = width * devices
    gain = norm_train.shape[0]
    layers = cols // 2
    rows = devices * cols * gain // 128
    hbm = pl.BlockSpec(memory_space=pltpu.HBM)
    vmem = pl.BlockSpec(memory_space=pltpu.VMEM)
    dma = pltpu.SemaphoreType.DMA
    out_g, out_u, factor, norm = pl.pallas_call(
        functools.partial(kernel, layers, rows_total),
        out_shape=(
            pltpu.VMEM((wide, rows_total), BF16),
            pltpu.VMEM((wide, rows_total), BF16),
            jax.ShapeDtypeStruct((2, padded), F32),
            jax.ShapeDtypeStruct((rows, 128), BF16),
        ),
        in_specs=[hbm] * 8,
        out_specs=[vmem] * 4,
        scratch_shapes=[
            pltpu.VMEM((2, devices, 1, 128), F32),
            pltpu.VMEM((layers, devices, 128), F32),
            pltpu.VMEM((rows, 128), F32),
            pltpu.VMEM((2, 1, gain), F32),
            pltpu.VMEM((2, wide, width), BF16),
            pltpu.VMEM((2, rank, width), BF16),
            pltpu.VMEM((2, rank, wide), BF16),
            pltpu.VMEM((2, 2, wide, width), BF16),
            pltpu.VMEM((2, 2, rank, width), BF16),
            pltpu.VMEM((2, wide, width), F32),
            pltpu.VMEM((2, padded, width // 2), F32),
            pltpu.VMEM((2, padded, 128), F32),
            pltpu.VMEM((SIDE, 2, padded), F32),
            pltpu.VMEM((SIDE, 2, padded), F32),
            dma((2,)), dma((2, 3)),
            dma((2, 2, 4)), dma((2, 2, 4)),
            dma((2, 2)), dma((2, 2)),
            dma((2, 2)), dma((2, 2)),
            dma((2, 2, 3)), dma((2, 2, 3)),
            dma((2, 2)), dma((2, 2)),
            dma((5, 3)), dma((5, 3)),
            dma((layers,)), dma((layers,)),
        ],
        compiler_params=pltpu.CompilerParams(
            collective_id=0, has_side_effects=True, vmem_limit_bytes=24 * 1024 * 1024
        ),
    )(
        *(
            pltpu.with_memory_space_constraint(array, pltpu.HBM)
            for array in (
                train_gate.T, train_up.T, low_gate.T, low_up.T, high_gate, high_up,
                norm_train.reshape(1, -1), norm_step.reshape(1, -1),
            )
        )
    )
    whole = jax.ShapeDtypeStruct((wide, rows_total), BF16)
    ready_g, ready_u, factor_g, factor_u, norm = pl.pallas_call(
        functools.partial(put, width),
        out_shape=(
            whole,
            whole,
            jax.ShapeDtypeStruct((wide,), F32),
            jax.ShapeDtypeStruct((wide,), F32),
            jax.ShapeDtypeStruct((rows, 128), BF16),
        ),
        in_specs=[vmem] * 4,
        out_specs=[hbm] * 2 + [vmem] * 3,
        scratch_shapes=[dma((2, 4, 4))],
        compiler_params=pltpu.CompilerParams(vmem_limit_bytes=1024 * 1024),
    )(out_g, out_u, factor, norm)
    tail = pl.pallas_call(
        last_relays,
        out_shape=pltpu.VMEM((2, wide, SIDE * width), BF16),
        in_specs=[vmem] * 2 + [hbm],
        out_specs=vmem,
        scratch_shapes=[dma((2, 2)), dma((2, 2))],
        compiler_params=pltpu.CompilerParams(
            collective_id=1, has_side_effects=True, vmem_limit_bytes=1024 * 1024
        ),
    )(out_g, out_u, pltpu.with_memory_space_constraint(norm, pltpu.HBM))
    ready_g, ready_u = pl.pallas_call(
        put_tail,
        out_shape=(whole, whole),
        in_specs=[vmem, hbm, hbm],
        out_specs=[hbm] * 2,
        input_output_aliases={1: 0, 2: 1},
        scratch_shapes=[dma((2, 4))],
        compiler_params=pltpu.CompilerParams(vmem_limit_bytes=1024 * 1024),
    )(tail, ready_g, ready_u)
    return ready_g.T, ready_u.T, factor_g, factor_u, norm.reshape(-1)


def solution(mesh):
    return jax.shard_map(
        functools.partial(shards, mesh.shape["zero"], mesh.shape["cols"]),
        mesh=mesh,
        in_specs=(
            P("zero", "cols"),
            P("zero", None),
            P(None, "cols"),
            P("zero", "cols"),
            P("zero", None),
            P(None, "cols"),
            P(("zero", "cols")),
            P(("zero", "cols")),
        ),
        out_specs=(P(None, "cols"), P(None, "cols"), P("cols"), P("cols"), P()),
        check_vma=False,
    )
```
